64 devices in a mesh: dp: 4 (over x, y), sp: 16 (over z, core).
Axes of the slice: x: 2, y: 2, z: 8, core: 2. Of those that a mesh axis runs over, the one named last changes fastest.
The devices are a block of a 4x4x8 slice.
Arguments:
- hidden: bfloat16 [512, 6144], P('dp'), parts along dimension 0
- w_norm: bfloat16 [6144], replicated
- w_q: bfloat16 [6144, 6144], replicated
- w_k: bfloat16 [6144, 128], replicated
- w_v: bfloat16 [6144, 128], replicated
- w_o: bfloat16 [6144, 6144], replicated
- k_cache: bfloat16 [512, 2048, 128], P('dp', 'sp'), parts along dimension 0
- v_cache: bfloat16 [512, 2048, 128], P('dp', 'sp'), parts along dimension 0
- cache_len: int32 [512], P('dp'), parts along dimension 0
Outputs:
- output 1: bfloat16 [512, 6144], P('dp'), parts along dimension 0
- output 2: bfloat16 [512, 2048, 128], P('dp', 'sp'), parts along dimension 0
- output 3: bfloat16 [512, 2048, 128], P('dp', 'sp'), parts along dimension 0
There are 4 independent parts. The reference program is written for one: setup_inputs(seed, part) draws one part's arguments, and reference() takes and returns one part's arrays. A program takes and returns all parts, laid end to end along the dimension named above; an argument that names none is the same for every part.
All inputs are finite; a program needn't handle non-finite values.
Results may differ from the reference program's by a relative error of at most 0.0151788.
Values sent between devices are 32-bit elements.
A program may use at most 768 MiB of HBM per device.

```python
import math
import jax
import jax.numpy as jnp
from jax import lax

D = 6144
HEADS = 48
HEAD = 128
ROWS = 128
SEQ = 2048

ROPE_BASE = 10000.0
EPSILON = 1e-6


def rotate_half(vectors, cos_t, sin_t):
    half_dim = vectors.shape[-1] // 2
    lower_half = vectors[..., :half_dim]
    upper_half = vectors[..., half_dim:]
    return jnp.concatenate([lower_half * cos_t - upper_half * sin_t, upper_half * cos_t + lower_half * sin_t], axis=-1)


def setup_inputs(seed: int = 0, part: int = 0) -> dict:
    base_key = jax.random.key(seed)
    shared_keys = jax.random.split(base_key, 5)
    part_keys = jax.random.split(jax.random.fold_in(base_key, part), 5)
    width = HEADS * HEAD
    score_spread = math.sqrt(max(math.log(SEQ / 16.0), 1.0))
    align = (1.5 * math.log(SEQ) - 3.5) * HEADS / math.sqrt(HEAD)
    hidden = jax.random.normal(part_keys[0], (ROWS, D), jnp.float32)
    w_norm = 0.5 * jax.random.normal(shared_keys[0], (D,), jnp.float32)
    w_q = jax.random.normal(shared_keys[1], (D, width), jnp.float32) * D ** -0.5
    q_mean = w_q.reshape(D, HEADS, HEAD).mean(axis=1)
    w_k = align * q_mean + jax.random.normal(shared_keys[2], (D, HEAD), jnp.float32) * D ** -0.5
    w_v = jax.random.normal(shared_keys[3], (D, HEAD), jnp.float32) * D ** -0.5
    w_o = jax.random.normal(shared_keys[4], (width, D), jnp.float32) * (3.0 * width ** -0.5)
    key_scale = score_spread * jax.random.uniform(part_keys[1], (ROWS, SEQ, 1), jnp.float32, minval=0.5, maxval=1.5)
    k_cache = jax.random.normal(part_keys[2], (ROWS, SEQ, HEAD), jnp.float32) * key_scale
    v_cache = jax.random.normal(part_keys[3], (ROWS, SEQ, HEAD), jnp.float32)
    row_ids = jnp.arange(ROWS)
    lengths = jax.random.randint(part_keys[4], (ROWS,), SEQ // 8, SEQ)
    lengths = jnp.where(row_ids == 0, SEQ - 1, jnp.where(row_ids == ROWS - 1, SEQ // 8, lengths))
    return {'hidden': hidden.astype(jnp.bfloat16), 'w_norm': w_norm.astype(jnp.bfloat16), 'w_q': w_q.astype(jnp.bfloat16), 'w_k': w_k.astype(jnp.bfloat16), 'w_v': w_v.astype(jnp.bfloat16), 'w_o': w_o.astype(jnp.bfloat16), 'k_cache': k_cache.astype(jnp.bfloat16), 'v_cache': v_cache.astype(jnp.bfloat16), 'cache_len': lengths.astype(jnp.int32)}


def reference(hidden, w_norm, w_q, w_k, w_v, w_o, k_cache, v_cache, cache_len):
    x_f32 = hidden.astype(jnp.float32)
    inv_rms = lax.rsqrt(jnp.mean(x_f32 * x_f32, axis=-1, keepdims=True) + EPSILON)
    x_norm = (x_f32 * inv_rms * (1.0 + w_norm.astype(jnp.float32))).astype(jnp.bfloat16)
    q_proj = jnp.dot(x_norm, w_q, preferred_element_type=jnp.float32).astype(jnp.bfloat16)
    k_proj = jnp.dot(x_norm, w_k, preferred_element_type=jnp.float32).astype(jnp.bfloat16)
    v_proj = jnp.dot(x_norm, w_v, preferred_element_type=jnp.float32).astype(jnp.bfloat16)
    inv_freq = ROPE_BASE ** (-jnp.arange(HEAD // 2, dtype=jnp.float32) * 2.0 / HEAD)
    angles = cache_len.astype(jnp.float32)[:, None] * inv_freq[None, :]
    cos_t = jnp.cos(angles)
    sin_t = jnp.sin(angles)
    q_heads = q_proj.astype(jnp.float32).reshape(ROWS, HEADS, HEAD)
    q_rot = (rotate_half(q_heads, cos_t[:, None, :], sin_t[:, None, :]) * HEAD ** -0.5).astype(jnp.bfloat16)
    k_rot = rotate_half(k_proj.astype(jnp.float32), cos_t, sin_t).astype(jnp.bfloat16)
    positions = jnp.arange(SEQ)
    at_slot = (positions[None, :] == cache_len[:, None])[:, :, None]
    new_k_cache = jnp.where(at_slot, k_rot[:, None, :], k_cache)
    new_v_cache = jnp.where(at_slot, v_proj[:, None, :], v_cache)

    def one_row(row_args):
        q_row, k_row, v_row, length = row_args
        scores = jnp.einsum('hd,td->ht', q_row.astype(jnp.float32), k_row.astype(jnp.float32))
        scores = jnp.where(positions[None, :] <= length, scores, -jnp.inf)
        weights = jax.nn.softmax(scores, axis=-1)
        return jnp.einsum('ht,td->hd', weights, v_row.astype(jnp.float32))

    attended = lax.map(one_row, (q_rot, new_k_cache, new_v_cache, cache_len))
    attended = attended.reshape(ROWS, HEADS * HEAD).astype(jnp.bfloat16)
    out_hidden = x_f32 + jnp.dot(attended, w_o, preferred_element_type=jnp.float32)
    return out_hidden.astype(jnp.bfloat16), new_k_cache, new_v_cache
```

```python
import functools

import jax
import jax.numpy as jnp
import numpy as np
from jax import lax
from jax.experimental import pallas as pl
from jax.experimental.pallas import tpu as pltpu
from jax.sharding import PartitionSpec as P

ROPE_BASE = 10000.0
EPSILON = 1e-6
MIB = 1024 * 1024
F32 = jnp.float32
BF16 = jnp.bfloat16
FLOOR = float(np.finfo(np.float32).min)
MESH = pl.DeviceIdType.MESH
ROW_BLOCK = 8
PROJ_SLOTS = 4
OUT_SLOTS = 4
OUT_TILE = 512


def remote(src, dst, send_sem, recv_sem, device):
    return pltpu.make_async_remote_copy(src_ref=src, dst_ref=dst, send_sem=send_sem, recv_sem=recv_sem, device_id={'sp': device}, device_id_type=MESH)


def enter(devices):
    barrier = pltpu.get_barrier_semaphore()
    for device in devices:
        pl.semaphore_signal(barrier, inc=1, device_id={'sp': device}, device_id_type=MESH)
    pl.semaphore_wait(barrier, len(devices))


def project_kernel(x_ref, w_norm_ref, cos_ref, sin_ref, w_q_ref, w_k_ref, w_v_ref, q_ref, k_ref, v_ref, x_norm, w_buf, w_sem, kv_sem, send_sem, recv_sem):
    me = lax.axis_index('sp')
    core = me % 2
    partner = me + 1 - 2 * core
    num_rows, width = x_ref.shape
    head = k_ref.shape[1]
    half = q_ref.shape[0] // 2
    pair = 2 * head
    num_blocks = half // 2
    first_head = core * half

    def fetch(block):
        slot = (block + 1) % PROJ_SLOTS
        columns = pl.ds(pl.multiple_of((first_head + 2 * block) * head, pair), pair)
        return pltpu.make_async_copy(w_q_ref.at[:, columns], w_buf.at[slot], w_sem.at[slot])

    fetch_k = pltpu.make_async_copy(w_k_ref, w_buf.at[0, :, pl.ds(0, head)], kv_sem.at[0])
    fetch_v = pltpu.make_async_copy(w_v_ref, w_buf.at[0, :, pl.ds(head, head)], kv_sem.at[1])
    fetch_k.start()
    fetch_v.start()
    for block in range(PROJ_SLOTS - 1):
        fetch(block).start()

    gain = 1.0 + w_norm_ref[...].astype(F32)

    def normalise(step, carry):
        rows = pl.ds(pl.multiple_of(step * 16, 16), 16)
        x = x_ref[rows, :].astype(F32)
        inv_rms = lax.rsqrt(jnp.mean(x * x, axis=-1, keepdims=True) + EPSILON)
        x_norm[rows, :] = (x * inv_rms * gain).astype(BF16)
        return carry

    lax.fori_loop(0, num_rows // 16, normalise, 0)
    cos_t = cos_ref[...]
    sin_t = sin_ref[...]

    def rotate(u):
        u = u.astype(BF16).astype(F32)
        return u * cos_t + pltpu.roll(u, head // 2, 1) * sin_t

    fetch_k.wait()
    fetch_v.wait()
    both = jnp.dot(x_norm[...], w_buf[0], preferred_element_type=F32)
    k_ref[...] = rotate(both[:, :head]).astype(BF16).astype(F32)
    v_ref[...] = both[:, head:].astype(BF16).astype(F32)
    fetch(PROJ_SLOTS - 1).start()
    enter([partner])

    def send(block):
        heads = q_ref.at[pl.ds(first_head + 2 * block, 2)]
        return remote(heads, heads, send_sem.at[block], recv_sem.at[block], partner)

    def step(block, carry):
        fetch(block).wait()
        product = jnp.dot(x_norm[...], w_buf[(block + 1) % PROJ_SLOTS], preferred_element_type=F32)

        @pl.when(block + PROJ_SLOTS < num_blocks)
        def _():
            fetch(block + PROJ_SLOTS).start()

        for i in range(2):
            q_ref[first_head + 2 * block + i] = (rotate(product[:, i * head:(i + 1) * head]) * head ** -0.5).astype(BF16).astype(F32)
        send(block).start()
        return carry

    lax.fori_loop(0, num_blocks, step, 0)

    def finish(block, carry):
        other = q_ref.at[pl.ds((1 - core) * half + 2 * block, 2)]
        remote(other, other, send_sem.at[block], recv_sem.at[block], partner).wait_recv()
        send(block).wait_send()
        return carry

    lax.fori_loop(0, num_blocks, finish, 0)


def project(hidden, w_norm, w_q, w_k, w_v, cache_len):
    num_rows, width = hidden.shape
    head = w_k.shape[1]
    heads = w_q.shape[1] // head
    inv_freq = jnp.asarray(ROPE_BASE ** (-np.arange(head // 2) * 2.0 / head), F32)
    angles = cache_len.astype(F32)[:, None] * jnp.concatenate([inv_freq, inv_freq])[None, :]
    sign = jnp.asarray(np.where(np.arange(head) < head // 2, -1.0, 1.0), F32)
    vmem = pl.BlockSpec(memory_space=pltpu.VMEM)
    hbm = pl.BlockSpec(memory_space=pl.ANY)
    blocks = heads // 4
    return pl.pallas_call(
        project_kernel,
        name='project',
        out_shape=(jax.ShapeDtypeStruct((heads, num_rows, head), F32), jax.ShapeDtypeStruct((num_rows, head), F32), jax.ShapeDtypeStruct((num_rows, head), F32)),
        in_specs=[vmem, vmem, vmem, vmem, hbm, hbm, hbm],
        out_specs=(vmem, vmem, vmem),
        scratch_shapes=[
            pltpu.VMEM((num_rows, width), BF16),
            pltpu.VMEM((PROJ_SLOTS, width, 2 * head), BF16),
            pltpu.SemaphoreType.DMA((PROJ_SLOTS,)),
            pltpu.SemaphoreType.DMA((2,)),
            pltpu.SemaphoreType.DMA((blocks,)),
            pltpu.SemaphoreType.DMA((blocks,)),
        ],
        compiler_params=pltpu.CompilerParams(collective_id=0, has_side_effects=True, vmem_limit_bytes=40 * MIB),
    )(hidden, w_norm.reshape(1, -1), jnp.cos(angles), jnp.sin(angles) * sign, w_q, w_k, w_v)


def attend_kernel(len_ref, q_ref, k_new_ref, v_new_ref, k_ref, v_ref, k_out, v_out, num_ref, stat_ref, staged):
    heads, rows, head = q_ref.shape
    slots = k_ref.shape[1]
    base = lax.axis_index('sp') * slots
    queries = q_ref.reshape(heads * rows, head)
    group_iota = lax.broadcasted_iota(jnp.int32, (16, head), 0)
    lane_iota = lax.broadcasted_iota(jnp.int32, (heads, slots), 1)
    for r in range(rows):
        row = pl.program_id(0) * rows + r
        p = len_ref[row] - base
        group = pl.multiple_of(jnp.clip(p, 0, slots - 1) // 16 * 16, 16)
        for new, old, out in ((k_new_ref, k_ref, k_out), (v_new_ref, v_ref, v_out)):
            out[r] = old[r]
            tile = old[r, pl.ds(group, 16), :].astype(F32)
            out[r, pl.ds(group, 16), :] = jnp.where(group_iota == p - group, new[r:r + 1, :], tile).astype(BF16)
        q = queries[pl.ds(r, heads, stride=rows), :].astype(BF16)
        scores = lax.dot_general(q, k_out[r], (((1,), (1,)), ((), ())), preferred_element_type=F32)
        valid = lane_iota <= p
        scores = jnp.where(valid, scores, FLOOR)
        row_max = jnp.max(scores, axis=1, keepdims=True)
        weights = jnp.where(valid, jnp.exp(scores - row_max), 0.0)
        total = jnp.sum(weights, axis=1, keepdims=True)
        staged[pl.ds(r, heads, stride=rows), :] = jnp.dot(weights.astype(BF16), v_out[r], preferred_element_type=F32)
        here = lane_iota == row
        stat_ref[0:heads, :] = jnp.where(here, row_max, stat_ref[0:heads, :])
        stat_ref[heads:2 * heads, :] = jnp.where(here, total, stat_ref[heads:2 * heads, :])
    num_ref[...] = staged[...].reshape(heads, rows, head)


def attend(q, k_new, v_new, k_block, v_block, cache_len):
    heads, num_rows, head = q.shape
    slots = k_block.shape[1]
    rows = ROW_BLOCK
    by_head = pl.BlockSpec((heads, rows, head), lambda i, *_: (0, i, 0))
    by_row = pl.BlockSpec((rows, head), lambda i, *_: (i, 0))
    cache = pl.BlockSpec((rows, slots, head), lambda i, *_: (i, 0, 0))
    stats = pl.BlockSpec((2 * heads, num_rows), lambda i, *_: (0, 0))
    return pl.pallas_call(
        attend_kernel,
        name='attend',
        out_shape=(jax.ShapeDtypeStruct(k_block.shape, BF16), jax.ShapeDtypeStruct(v_block.shape, BF16), jax.ShapeDtypeStruct(q.shape, F32), jax.ShapeDtypeStruct((2 * heads, num_rows), F32)),
        grid_spec=pltpu.PrefetchScalarGridSpec(
            num_scalar_prefetch=1,
            grid=(num_rows // rows,),
            in_specs=[by_head, by_row, by_row, cache, cache],
            out_specs=(cache, cache, by_head, stats),
            scratch_shapes=[pltpu.VMEM((heads * rows, head), F32)],
        ),
        compiler_params=pltpu.CompilerParams(dimension_semantics=('arbitrary',), vmem_limit_bytes=32 * MIB),
    )(cache_len, q, k_new, v_new, k_block, v_block)


def combine_kernel(nz, num_ref, stat_ref, x_ref, w_o_ref, out_ref, near_num, near_stat, part, from_long, from_short, gathered, total, attended, w_buf, w_sem, stat_sem, near_send, near_recv, long_send, long_recv, short_send, short_recv, far_send, far_recv, back_send, back_recv, side_send, side_recv):
    me = lax.axis_index('sp')
    z = me // 2
    core = me % 2
    partner = me + 1 - 2 * core
    way = 1 - 2 * core
    heads, num_rows, head = num_ref.shape
    share = heads // (2 * nz)
    far = nz // 2
    width = out_ref.shape[1]
    depth = 2 * share * head

    def device(chip, c):
        return (chip + 2 * nz) % nz * 2 + c

    ahead = device(z + way, core)
    behind = device(z - way, core)
    targets = [far]
    for hop in range(far - 1, 0, -1):
        targets += [-hop, hop]
    targets.append(0)
    sources = [0]
    for hop in range(1, far):
        sources += [-hop, hop]
    sources.append(-far)

    def fetch(k):
        chip = device(z + way * sources[k], 0) // 2
        return pltpu.make_async_copy(w_o_ref.at[pl.ds(pl.multiple_of(chip * depth, depth), depth), :], w_buf.at[k % OUT_SLOTS], w_sem.at[k % OUT_SLOTS])

    for k in range(OUT_SLOTS):
        fetch(k).start()
    enter([partner, ahead, behind])

    swap_stat = remote(stat_ref, near_stat, stat_sem.at[0], stat_sem.at[1], partner)
    swap_stat.start()
    swaps = []
    for i, hop in enumerate(targets):
        first = share * device(z - way * hop, 1 - core)
        swap = remote(num_ref.at[pl.ds(first, share)], near_num.at[i], near_send.at[i], near_recv.at[i], partner)
        swap.start()
        swaps.append(swap)

    def column(row):
        return jnp.broadcast_to(row, (num_rows, num_rows)).T

    def merge(a, b):
        (x_a, m_a, l_a), (x_b, m_b, l_b) = a, b
        m = jnp.maximum(m_a, m_b)
        scale_a = jnp.exp(m_a - m)
        scale_b = jnp.exp(m_b - m)
        return x_a * column(scale_a) + x_b * column(scale_b), m, l_a * scale_a + l_b * scale_b

    def load(ref):
        return ref[0:num_rows, :], ref[num_rows:num_rows + 1, :], ref[num_rows + 1:num_rows + 2, :]

    sub_iota = lax.broadcasted_iota(jnp.int32, (8, num_rows), 0)

    def store(ref, triple):
        x, m, l = triple
        ref[0:num_rows, :] = x
        ref[num_rows:num_rows + 8, :] = jnp.where(sub_iota == 0, m, l)

    def own(i):
        swaps[i].wait_recv()
        first = share * device(z + way * targets[i], core)
        for s in range(share):
            h = first + s
            mine = (num_ref[h], stat_ref[pl.ds(h, 1), :], stat_ref[pl.ds(heads + h, 1), :])
            theirs = (near_num[i, s], near_stat[pl.ds(h, 1), :], near_stat[pl.ds(heads + h, 1), :])
            store(part.at[i, s], merge(mine, theirs))

    def long_copy(hop, s):
        i = 0 if hop == 0 else 2 * hop
        return remote(part.at[i, s], from_long.at[hop, s], long_send.at[hop, s], long_recv.at[hop, s], ahead)

    def short_copy(hop, s):
        return remote(part.at[2 * hop + 1, s], from_short.at[hop, s], short_send.at[hop, s], short_recv.at[hop, s], behind)

    swap_stat.wait_recv()
    for hop in range(far):
        own(2 * hop)
        if hop == 0:
            for s in range(share):
                long_copy(0, s).start()
        own(2 * hop + 1)
        if hop == 0:
            for s in range(share):
                short_copy(0, s).start()
            continue
        for s in range(share):
            long_copy(hop - 1, s).wait_recv()
            store(part.at[2 * hop, s], merge(load(part.at[2 * hop, s]), load(from_long.at[hop - 1, s])))
            long_copy(hop, s).start()
            if hop < far - 1:
                short_copy(hop - 1, s).wait_recv()
                store(part.at[2 * hop + 1, s], merge(load(part.at[2 * hop + 1, s]), load(from_short.at[hop - 1, s])))
                short_copy(hop, s).start()

    def far_copy(hop, s):
        slot = gathered.at[device(z - way * hop, core), s]
        return remote(slot, slot, far_send.at[hop, s], far_recv.at[hop, s], ahead)

    def back_copy(hop, s):
        slot = gathered.at[device(z + way * hop, core), s]
        return remote(slot, slot, back_send.at[hop, s], back_recv.at[hop, s], behind)

    def side_copy(k, s):
        slot = gathered.at[device(z + way * sources[k], core), s]
        return remote(slot, slot, side_send.at[k, s], side_recv.at[k, s], partner)

    def far_arrival(hop, s):
        slot = gathered.at[device(z - way * (hop + 1), core), s]
        return remote(slot, slot, far_send.at[hop, s], far_recv.at[hop, s], ahead)

    def back_arrival(hop, s):
        slot = gathered.at[device(z + way * (hop + 1), core), s]
        return remote(slot, slot, back_send.at[hop, s], back_recv.at[hop, s], behind)

    def side_arrival(k, s):
        slot = gathered.at[device(z - way * sources[k], 1 - core), s]
        return remote(slot, slot, side_send.at[k, s], side_recv.at[k, s], partner)

    mirror = {hop: k for k, hop in enumerate(sources)}
    mirror[far] = mirror[-far]

    last = far - 1
    for s in range(share):
        short_copy(last - 1, s).wait_recv()
        triple = merge(load(part.at[2 * far - 1, s]), load(from_short.at[last - 1, s]))
        long_copy(last, s).wait_recv()
        x, _, l = merge(triple, load(from_long.at[last, s]))
        gathered[me, s] = (x / column(l)).astype(BF16).astype(F32)
        far_copy(0, s).start()
        back_copy(0, s).start()
        side_copy(0, s).start()

    tiles = width // OUT_TILE

    def prepare(k):
        for s in range(share):
            side_arrival(mirror[-sources[k]], s).wait_recv()
        chip = z + way * sources[k]
        for c in range(2):
            for s in range(share):
                attended[:, (c * share + s) * head:(c * share + s + 1) * head] = gathered[device(chip, c), s].astype(BF16)
        fetch(k).wait()

    def multiply(k, low, high):
        def tile(n, carry):
            columns = pl.ds(pl.multiple_of(n * OUT_TILE, OUT_TILE), OUT_TILE)
            product = jnp.dot(attended[...], w_buf[k % OUT_SLOTS, :, columns], preferred_element_type=F32)
            if k == 0:
                total[:, columns] = product
            elif k < nz - 1:
                total[:, columns] = total[:, columns] + product
            else:
                out_ref[:, columns] = (x_ref[:, columns].astype(F32) + (total[:, columns] + product)).astype(BF16)
            return carry

        lax.fori_loop(low, high, tile, 0)
        if high == tiles and k + OUT_SLOTS < nz:
            fetch(k + OUT_SLOTS).start()

    pending = [0]
    for hop in range(far):
        work = [(k, n) for k in pending for n in range(2)]
        for s in range(share):
            far_arrival(hop, s).wait_recv()
            if hop < far - 1:
                far_copy(hop + 1, s).start()
            side_copy(mirror[-(hop + 1)], s).start()
            if hop < far - 1:
                back_arrival(hop, s).wait_recv()
                if hop < far - 2:
                    back_copy(hop + 1, s).start()
                side_copy(mirror[hop + 1], s).start()
            count = -(-len(work) // (share - s))
            for k, n in work[:count]:
                if n == 0:
                    prepare(k)
                multiply(k, n * tiles // 2, (n + 1) * tiles // 2)
            work = work[count:]
        pending = [mirror[-(hop + 1)]] + ([mirror[hop + 1]] if hop < far - 1 else [])
    for k in pending:
        prepare(k)
        multiply(k, 0, tiles)

    swap_stat.wait_send()
    for swap in swaps:
        swap.wait_send()
    for s in range(share):
        for hop in range(far):
            long_copy(hop, s).wait_send()
            far_copy(hop, s).wait_send()
            if hop < far - 1:
                short_copy(hop, s).wait_send()
                back_copy(hop, s).wait_send()
        for k in range(nz):
            side_copy(k, s).wait_send()


def combine(num, stat, hidden, w_o, group):
    heads, num_rows, head = num.shape
    nz = group // 2
    share = heads // group
    far = nz // 2
    width = w_o.shape[1]
    vmem = pl.BlockSpec(memory_space=pltpu.VMEM)
    hbm = pl.BlockSpec(memory_space=pl.ANY)
    dma = pltpu.SemaphoreType.DMA
    piece = (num_rows + 8, head)
    return pl.pallas_call(
        functools.partial(combine_kernel, nz),
        name='combine',
        out_shape=jax.ShapeDtypeStruct((num_rows, width), BF16),
        in_specs=[vmem, vmem, vmem, hbm],
        out_specs=vmem,
        scratch_shapes=[
            pltpu.VMEM((nz, share, num_rows, head), F32),
            pltpu.VMEM((2 * heads, num_rows), F32),
            pltpu.VMEM((nz, share) + piece, F32),
            pltpu.VMEM((far, share) + piece, F32),
            pltpu.VMEM((far - 1, share) + piece, F32),
            pltpu.VMEM((group, share, num_rows, head), F32),
            pltpu.VMEM((num_rows, width), F32),
            pltpu.VMEM((num_rows, 2 * share * head), BF16),
            pltpu.VMEM((OUT_SLOTS, 2 * share * head, width), BF16),
            dma((OUT_SLOTS,)),
            dma((2,)),
            dma((nz,)),
            dma((nz,)),
            dma((far, share)),
            dma((far, share)),
            dma((far - 1, share)),
            dma((far - 1, share)),
            dma((far, share)),
            dma((far, share)),
            dma((far - 1, share)),
            dma((far - 1, share)),
            dma((nz, share)),
            dma((nz, share)),
        ],
        compiler_params=pltpu.CompilerParams(collective_id=1, has_side_effects=True, vmem_limit_bytes=62 * MIB),
    )(num, stat, hidden, w_o)


def solution(mesh):
    group = mesh.shape['sp']

    def local_step(hidden, w_norm, w_q, w_k, w_v, w_o, k_block, v_block, cache_len):
        q, k_new, v_new = project(hidden, w_norm, w_q, w_k, w_v, cache_len)
        k_out, v_out, num, stat = attend(q, k_new, v_new, k_block, v_block, cache_len)
        out = combine(num, stat, hidden, w_o, group)
        return out, k_out, v_out

    cache_spec = P('dp', 'sp', None)
    return jax.shard_map(local_step, mesh=mesh, in_specs=(P('dp', None), P(None), P(None, None), P(None, None), P(None, None), P(None, None), cache_spec, cache_spec, P('dp')), out_specs=(P('dp', None), cache_spec, cache_spec), check_vma=False)
```

```python
import functools

import jax
import jax.numpy as jnp
import numpy as np
from jax import lax
from jax.experimental import pallas as pl
from jax.experimental.pallas import tpu as pltpu
from jax.sharding import PartitionSpec as P

ROPE_BASE = 10000.0
EPSILON = 1e-6
MIB = 1024 * 1024
F32 = jnp.float32
BF16 = jnp.bfloat16
FLOOR = float(np.finfo(np.float32).min)
MESH = pl.DeviceIdType.MESH
TURN = (6.28125, 0.0019340515136718750, float(2 * np.pi - 6.28125 - 0.0019340515136718750))
ROW_BLOCK = 8
PROJ_SLOTS = 4
OUT_SLOTS = 4
OUT_TILE = 1536


def remote(src, dst, send_sem, recv_sem, device):
    return pltpu.make_async_remote_copy(src_ref=src, dst_ref=dst, send_sem=send_sem, recv_sem=recv_sem, device_id={'sp': device}, device_id_type=MESH)


def enter(devices):
    barrier = pltpu.get_barrier_semaphore()
    for device in devices:
        pl.semaphore_signal(barrier, inc=1, device_id={'sp': device}, device_id_type=MESH)
    pl.semaphore_wait(barrier, len(devices))


def project_kernel(freq_ref, len_ref, w_norm_ref, x_hbm, w_q_ref, w_k_ref, w_v_ref, q_ref, k_ref, v_ref, x_ref, x_norm, w_buf, q_buf, x_sem, w_sem, kv_sem, out_sem, send_sem, recv_sem):
    me = lax.axis_index('sp')
    core = me % 2
    partner = me + 1 - 2 * core
    num_rows, width = x_ref.shape
    head = k_ref.shape[1]
    half = q_ref.shape[1] // ROW_BLOCK // 2
    pair = 2 * head
    num_blocks = half // 2
    first_head = core * half

    def fetch(block):
        slot = (block + 1) % PROJ_SLOTS
        columns = pl.ds(pl.multiple_of((first_head + 2 * block) * head, pair), pair)
        return pltpu.make_async_copy(w_q_ref.at[:, columns], w_buf.at[slot], w_sem.at[slot])

    fetch_k = pltpu.make_async_copy(w_k_ref, w_buf.at[0, :, pl.ds(0, head)], kv_sem.at[0])
    fetch_v = pltpu.make_async_copy(w_v_ref, w_buf.at[0, :, pl.ds(head, head)], kv_sem.at[1])
    fetch_x = pltpu.make_async_copy(x_hbm, x_ref, x_sem.at[0])
    fetch_x.start()
    fetch_k.start()
    fetch_v.start()
    for block in range(PROJ_SLOTS - 1):
        fetch(block).start()

    gain = 1.0 + w_norm_ref[...].astype(F32)
    angles = jnp.broadcast_to(len_ref[...].astype(F32), (num_rows, num_rows)).T * freq_ref[...]
    turns = jnp.round(angles * (0.5 / np.pi))
    for part in TURN:
        angles = angles - turns * part
    cos_t = jnp.cos(angles)
    sin_t = jnp.where(lax.broadcasted_iota(jnp.int32, angles.shape, 1) < head // 2, -1.0, 1.0) * jnp.sin(angles)
    fetch_x.wait()

    def normalise(step, carry):
        rows = pl.ds(pl.multiple_of(step * 16, 16), 16)
        x = x_ref[rows, :].astype(F32)
        inv_rms = lax.rsqrt(jnp.mean(x * x, axis=-1, keepdims=True) + EPSILON)
        x_norm[rows, :] = (x * inv_rms * gain).astype(BF16)
        return carry

    lax.fori_loop(0, num_rows // 16, normalise, 0)

    def rotate(u):
        u = u.astype(BF16).astype(F32)
        return u * cos_t + pltpu.roll(u, head // 2, 1) * sin_t

    fetch_k.wait()
    fetch_v.wait()
    both = jnp.dot(x_norm[...], w_buf[0], preferred_element_type=F32)
    k_ref[...] = rotate(both[:, :head]).astype(BF16).astype(F32)
    v_ref[...] = both[:, head:].astype(BF16).astype(F32)
    fetch(PROJ_SLOTS - 1).start()
    enter([partner])

    def heads_of(c, block):
        rows = pl.multiple_of((c * half + 2 * block) * ROW_BLOCK, 2 * ROW_BLOCK)
        return q_ref.at[:, pl.ds(rows, 2 * ROW_BLOCK), :]

    def keep(block):
        return pltpu.make_async_copy(q_buf.at[block], heads_of(core, block), out_sem.at[block])

    def send(block):
        return remote(q_buf.at[block], heads_of(core, block), send_sem.at[block], recv_sem.at[block], partner)

    def step(block, carry):
        fetch(block).wait()
        product = jnp.dot(x_norm[...], w_buf[(block + 1) % PROJ_SLOTS], preferred_element_type=F32)

        @pl.when(block + PROJ_SLOTS < num_blocks)
        def _():
            fetch(block + PROJ_SLOTS).start()

        for i in range(2):
            q = (rotate(product[:, i * head:(i + 1) * head]) * head ** -0.5).astype(BF16).astype(F32)
            q_buf[block, :, i * ROW_BLOCK:(i + 1) * ROW_BLOCK, :] = q.reshape(num_rows // ROW_BLOCK, ROW_BLOCK, head)
        send(block).start()
        keep(block).start()
        return carry

    lax.fori_loop(0, num_blocks, step, 0)

    def finish(block, carry):
        keep(block).wait()
        send(block).wait_send()
        other = heads_of(1 - core, block)
        remote(q_buf.at[block], other, send_sem.at[block], recv_sem.at[block], partner).wait_recv()
        return carry

    lax.fori_loop(0, num_blocks, finish, 0)


def project(hidden, w_norm, w_q, w_k, w_v, cache_len):
    num_rows, width = hidden.shape
    head = w_k.shape[1]
    heads = w_q.shape[1] // head
    inv_freq = ROPE_BASE ** (-np.arange(head // 2) * 2.0 / head)
    inv_freq = jnp.asarray(np.concatenate([inv_freq, inv_freq])[None, :], F32)
    vmem = pl.BlockSpec(memory_space=pltpu.VMEM)
    hbm = pl.BlockSpec(memory_space=pltpu.HBM)
    blocks = heads // 4
    return pl.pallas_call(
        project_kernel,
        name='project',
        out_shape=(jax.ShapeDtypeStruct((num_rows // ROW_BLOCK, heads * ROW_BLOCK, head), F32), jax.ShapeDtypeStruct((num_rows, head), F32), jax.ShapeDtypeStruct((num_rows, head), F32)),
        in_specs=[vmem, vmem, vmem, hbm, hbm, hbm, hbm],
        out_specs=(hbm, vmem, vmem),
        scratch_shapes=[
            pltpu.VMEM((num_rows, width), BF16),
            pltpu.VMEM((num_rows, width), BF16),
            pltpu.VMEM((PROJ_SLOTS, width, 2 * head), BF16),
            pltpu.VMEM((blocks, num_rows // ROW_BLOCK, 2 * ROW_BLOCK, head), F32),
            pltpu.SemaphoreType.DMA((1,)),
            pltpu.SemaphoreType.DMA((PROJ_SLOTS,)),
            pltpu.SemaphoreType.DMA((2,)),
            pltpu.SemaphoreType.DMA((blocks,)),
            pltpu.SemaphoreType.DMA((blocks,)),
            pltpu.SemaphoreType.DMA((blocks,)),
        ],
        compiler_params=pltpu.CompilerParams(collective_id=0, has_side_effects=True, vmem_limit_bytes=60 * MIB),
    )(inv_freq, cache_len.reshape(1, -1), w_norm, hidden, w_q, w_k, w_v)


def attend_kernel(len_ref, q_ref, k_new_ref, v_new_ref, k_ref, v_ref, k_out, v_out, num_ref, stat_ref, scores_ref):
    rows, slots, head = k_ref.shape
    heads = stat_ref.shape[0] // 2
    base = lax.axis_index('sp') * slots
    first = pl.program_id(0) * rows
    group_iota = lax.broadcasted_iota(jnp.int32, (16, head), 0)
    lane_iota = lax.broadcasted_iota(jnp.int32, (heads, slots), 1)
    places = [len_ref[first + r] - base for r in range(rows)]
    for new, old, out in ((k_new_ref, k_ref, k_out), (v_new_ref, v_ref, v_out)):
        out[...] = old[...]
        for r, p in enumerate(places):
            group = pl.multiple_of(jnp.clip(p, 0, slots - 1) // 16 * 16, 16)
            tile = old[r, pl.ds(group, 16), :].astype(F32)
            out[r, pl.ds(group, 16), :] = jnp.where(group_iota == p - group, new[r:r + 1, :], tile).astype(BF16)
    for r in range(rows):
        q = q_ref[pl.ds(r, heads, stride=rows), :].astype(BF16)
        scores_ref[r] = lax.dot_general(q, k_out[r], (((1,), (1,)), ((), ())), preferred_element_type=F32)
    maxima, totals, factors = [], [], []
    for r, p in enumerate(places):
        valid = lane_iota <= p
        scores = jnp.where(valid, scores_ref[r], FLOOR)
        row_max = jnp.max(scores, axis=1, keepdims=True)
        weights = jnp.where(valid, jnp.exp(scores - row_max), 0.0)
        maxima.append(row_max)
        totals.append(jnp.sum(weights, axis=1, keepdims=True))
        factors.append(weights.astype(BF16))
    for r in range(rows):
        num_ref[pl.ds(r, heads, stride=rows), :] = jnp.dot(factors[r], v_out[r], preferred_element_type=F32)
    stat_m = stat_ref[0:heads, :]
    stat_l = stat_ref[heads:2 * heads, :]
    for r in range(rows):
        here = lane_iota == first + r
        stat_m = jnp.where(here, maxima[r], stat_m)
        stat_l = jnp.where(here, totals[r], stat_l)
    stat_ref[0:heads, :] = stat_m
    stat_ref[heads:2 * heads, :] = stat_l


def attend(q, k_new, v_new, k_block, v_block, cache_len):
    num_rows, slots, head = k_block.shape
    rows = ROW_BLOCK
    heads = q.shape[1] // rows
    by_head = pl.BlockSpec((None, heads * rows, head), lambda i, *_: (i, 0, 0))
    by_row = pl.BlockSpec((rows, head), lambda i, *_: (i, 0))
    cache = pl.BlockSpec((rows, slots, head), lambda i, *_: (i, 0, 0))
    stats = pl.BlockSpec((2 * heads, num_rows), lambda i, *_: (0, 0))
    return pl.pallas_call(
        attend_kernel,
        name='attend',
        out_shape=(jax.ShapeDtypeStruct(k_block.shape, BF16), jax.ShapeDtypeStruct(v_block.shape, BF16), jax.ShapeDtypeStruct(q.shape, F32), jax.ShapeDtypeStruct((2 * heads, num_rows), F32)),
        grid_spec=pltpu.PrefetchScalarGridSpec(
            num_scalar_prefetch=1,
            grid=(num_rows // rows,),
            in_specs=[by_head, by_row, by_row, cache, cache],
            out_specs=(cache, cache, by_head, stats),
            scratch_shapes=[pltpu.VMEM((rows, heads, slots), F32)],
        ),
        compiler_params=pltpu.CompilerParams(dimension_semantics=('arbitrary',), vmem_limit_bytes=60 * MIB),
    )(cache_len, q, k_new, v_new, k_block, v_block)


def combine_kernel(nz, stat_ref, num_ref, x_hbm, w_o_ref, out_hbm, x_ref, out_ref, own_num, near_num, near_stat, part, from_long, from_short, gathered, total, attended, w_buf, x_sem, out_sem, own_sem, w_sem, stat_sem, near_send, near_recv, long_send, long_recv, short_send, short_recv, far_send, far_recv, back_send, back_recv, side_send, side_recv):
    me = lax.axis_index('sp')
    z = me // 2
    core = me % 2
    partner = me + 1 - 2 * core
    way = 1 - 2 * core
    num_rows, width = x_ref.shape
    heads = num_ref.shape[1] // ROW_BLOCK
    head = num_ref.shape[2]
    share = heads // (2 * nz)
    far = nz // 2
    depth = 2 * share * head

    def device(chip, c):
        return (chip + 2 * nz) % nz * 2 + c

    ahead = device(z + way, core)
    behind = device(z - way, core)
    targets = [far]
    for hop in range(far - 1, 0, -1):
        targets += [-hop, hop]
    targets.append(0)
    sources = [0]
    for hop in range(1, far):
        sources += [-hop, hop]
    sources.append(-far)

    def fetch(k):
        chip = device(z + way * sources[k], 0) // 2
        return pltpu.make_async_copy(w_o_ref.at[pl.ds(pl.multiple_of(chip * depth, depth), depth), :], w_buf.at[k % OUT_SLOTS], w_sem.at[k % OUT_SLOTS])

    def own_heads(i, c):
        way_c = way * (1 - 2 * c)
        rows = share * ROW_BLOCK
        first = rows * device(z + way_c * targets[i], core + way * c)
        return num_ref.at[:, pl.ds(pl.multiple_of(first, rows), rows), :]

    own_copies = [pltpu.make_async_copy(own_heads(i, 0), own_num.at[i], own_sem.at[i]) for i in range(nz)]
    for copy in own_copies:
        copy.start()
    enter([partner, ahead, behind])
    swap_stat = remote(stat_ref, near_stat, stat_sem.at[0], stat_sem.at[1], partner)
    swap_stat.start()
    swaps = []
    for i in range(nz):
        swap = remote(own_heads(i, 1), near_num.at[i], near_send.at[i], near_recv.at[i], partner)
        swap.start()
        swaps.append(swap)
    fetch_x = pltpu.make_async_copy(x_hbm, x_ref, x_sem.at[0])
    fetch_x.start()
    for k in range(OUT_SLOTS):
        fetch(k).start()

    def column(row):
        return jnp.broadcast_to(row, (num_rows, num_rows)).T

    def merge(a, b):
        (x_a, m_a, l_a), (x_b, m_b, l_b) = a, b
        m = jnp.maximum(m_a, m_b)
        scale_a = jnp.exp(m_a - m)
        scale_b = jnp.exp(m_b - m)
        return x_a * column(scale_a) + x_b * column(scale_b), m, l_a * scale_a + l_b * scale_b

    def load(ref):
        return ref[0:num_rows, :], ref[num_rows:num_rows + 1, :], ref[num_rows + 1:num_rows + 2, :]

    sub_iota = lax.broadcasted_iota(jnp.int32, (8, num_rows), 0)

    def store(ref, triple):
        x, m, l = triple
        ref[0:num_rows, :] = x
        ref[num_rows:num_rows + 8, :] = jnp.where(sub_iota == 0, m, l)

    def own(i):
        own_copies[i].wait()
        swaps[i].wait_recv()
        first = share * device(z + way * targets[i], core)
        for s in range(share):
            h = first + s
            mine = (own_num[i, :, s * ROW_BLOCK:(s + 1) * ROW_BLOCK, :].reshape(num_rows, head), stat_ref[pl.ds(h, 1), :], stat_ref[pl.ds(heads + h, 1), :])
            theirs = (near_num[i, :, s * ROW_BLOCK:(s + 1) * ROW_BLOCK, :].reshape(num_rows, head), near_stat[pl.ds(h, 1), :], near_stat[pl.ds(heads + h, 1), :])
            store(part.at[i, s], merge(mine, theirs))

    def long_copy(hop, s):
        i = 0 if hop == 0 else 2 * hop
        return remote(part.at[i, s], from_long.at[hop, s], long_send.at[hop, s], long_recv.at[hop, s], ahead)

    def short_copy(hop, s):
        return remote(part.at[2 * hop + 1, s], from_short.at[hop, s], short_send.at[hop, s], short_recv.at[hop, s], behind)

    swap_stat.wait_recv()
    for hop in range(far):
        own(2 * hop)
        if hop == 0:
            for s in range(share):
                long_copy(0, s).start()
        own(2 * hop + 1)
        if hop == 0:
            for s in range(share):
                short_copy(0, s).start()
            continue
        for s in range(share):
            long_copy(hop - 1, s).wait_recv()
            store(part.at[2 * hop, s], merge(load(part.at[2 * hop, s]), load(from_long.at[hop - 1, s])))
            long_copy(hop, s).start()
            if hop < far - 1:
                short_copy(hop - 1, s).wait_recv()
                store(part.at[2 * hop + 1, s], merge(load(part.at[2 * hop + 1, s]), load(from_short.at[hop - 1, s])))
                short_copy(hop, s).start()

    def far_copy(hop, s):
        slot = gathered.at[device(z - way * hop, core), s]
        return remote(slot, slot, far_send.at[hop, s], far_recv.at[hop, s], ahead)

    def back_copy(hop, s):
        slot = gathered.at[device(z + way * hop, core), s]
        return remote(slot, slot, back_send.at[hop, s], back_recv.at[hop, s], behind)

    def side_copy(k, s):
        slot = gathered.at[device(z + way * sources[k], core), s]
        return remote(slot, slot, side_send.at[k, s], side_recv.at[k, s], partner)

    def far_arrival(hop, s):
        slot = gathered.at[device(z - way * (hop + 1), core), s]
        return remote(slot, slot, far_send.at[hop, s], far_recv.at[hop, s], ahead)

    def back_arrival(hop, s):
        slot = gathered.at[device(z + way * (hop + 1), core), s]
        return remote(slot, slot, back_send.at[hop, s], back_recv.at[hop, s], behind)

    def side_arrival(k, s):
        slot = gathered.at[device(z - way * sources[k], 1 - core), s]
        return remote(slot, slot, side_send.at[k, s], side_recv.at[k, s], partner)

    mirror = {hop: k for k, hop in enumerate(sources)}
    mirror[far] = mirror[-far]

    last = far - 1
    for s in range(share):
        short_copy(last - 1, s).wait_recv()
        triple = merge(load(part.at[2 * far - 1, s]), load(from_short.at[last - 1, s]))
        long_copy(last, s).wait_recv()
        x, _, l = merge(triple, load(from_long.at[last, s]))
        gathered[me, s] = (x / column(l)).astype(BF16).astype(F32)
        far_copy(0, s).start()
        back_copy(0, s).start()
        side_copy(0, s).start()

    tiles = width // OUT_TILE

    def save(n):
        columns = pl.ds(pl.multiple_of(n * OUT_TILE, OUT_TILE), OUT_TILE)
        return pltpu.make_async_copy(out_ref.at[:, columns], out_hbm.at[:, columns], out_sem.at[n])

    def prepare(ks):
        for i, k in enumerate(ks):
            for s in range(share):
                side_arrival(mirror[-sources[k]], s).wait_recv()
            chip = z + way * sources[k]
            for c in range(2):
                for s in range(share):
                    column = i * depth + (c * share + s) * head
                    attended[:, column:column + head] = gathered[device(chip, c), s].astype(BF16)
            fetch(k).wait()

    def multiply(ks, n):
        columns = pl.ds(n * OUT_TILE, OUT_TILE)
        product = None
        for i, k in enumerate(ks):
            term = jnp.dot(attended[:, i * depth:(i + 1) * depth], w_buf[k % OUT_SLOTS, :, columns], preferred_element_type=F32)
            product = term if product is None else product + term
        if 0 in ks:
            total[:, columns] = product
        elif nz - 1 not in ks:
            total[:, columns] = total[:, columns] + product
        else:
            out_ref[:, columns] = (x_ref[:, columns].astype(F32) + (total[:, columns] + product)).astype(BF16)
            save(n).start()

    def release(ks):
        for k in ks:
            if k + OUT_SLOTS < nz:
                fetch(k + OUT_SLOTS).start()

    pending = [0]
    for hop in range(far):
        work = list(range(tiles))
        for s in range(share):
            far_arrival(hop, s).wait_recv()
            if hop < far - 1:
                far_copy(hop + 1, s).start()
            side_copy(mirror[-(hop + 1)], s).start()
            if hop < far - 1:
                back_arrival(hop, s).wait_recv()
                if hop < far - 2:
                    back_copy(hop + 1, s).start()
                side_copy(mirror[hop + 1], s).start()
            count = -(-len(work) // (share - s))
            for n in work[:count]:
                if n == 0:
                    prepare(pending)
                multiply(pending, n)
            work = work[count:]
        release(pending)
        pending = sorted(set([mirror[-(hop + 1)], mirror[hop + 1]]))
    fetch_x.wait()
    prepare(pending)
    for n in range(tiles):
        multiply(pending, n)
    for n in range(tiles):
        save(n).wait()

    swap_stat.wait_send()
    for swap in swaps:
        swap.wait_send()
    for s in range(share):
        for hop in range(far):
            long_copy(hop, s).wait_send()
            far_copy(hop, s).wait_send()
            if hop < far - 1:
                short_copy(hop, s).wait_send()
                back_copy(hop, s).wait_send()
        for k in range(nz):
            side_copy(k, s).wait_send()


def combine(num, stat, hidden, w_o, group):
    num_rows, width = hidden.shape
    heads = num.shape[1] // ROW_BLOCK
    head = num.shape[2]
    nz = group // 2
    share = heads // group
    far = nz // 2
    vmem = pl.BlockSpec(memory_space=pltpu.VMEM)
    hbm = pl.BlockSpec(memory_space=pltpu.HBM)
    dma = pltpu.SemaphoreType.DMA
    piece = (num_rows + 8, head)
    return pl.pallas_call(
        functools.partial(combine_kernel, nz),
        name='combine',
        out_shape=jax.ShapeDtypeStruct((num_rows, width), BF16),
        in_specs=[vmem, hbm, hbm, hbm],
        out_specs=hbm,
        scratch_shapes=[
            pltpu.VMEM((num_rows, width), BF16),
            pltpu.VMEM((num_rows, width), BF16),
            pltpu.VMEM((nz, num_rows // ROW_BLOCK, share * ROW_BLOCK, head), F32),
            pltpu.VMEM((nz, num_rows // ROW_BLOCK, share * ROW_BLOCK, head), F32),
            pltpu.VMEM((2 * heads, num_rows), F32),
            pltpu.VMEM((nz, share) + piece, F32),
            pltpu.VMEM((far, share) + piece, F32),
            pltpu.VMEM((far - 1, share) + piece, F32),
            pltpu.VMEM((group, share, num_rows, head), F32),
            pltpu.VMEM((num_rows, width), F32),
            pltpu.VMEM((num_rows, 4 * share * head), BF16),
            pltpu.VMEM((OUT_SLOTS, 2 * share * head, width), BF16),
            dma((1,)),
            dma((width // OUT_TILE,)),
            dma((nz,)),
            dma((OUT_SLOTS,)),
            dma((2,)),
            dma((nz,)),
            dma((nz,)),
            dma((far, share)),
            dma((far, share)),
            dma((far - 1, share)),
            dma((far - 1, share)),
            dma((far, share)),
            dma((far, share)),
            dma((far - 1, share)),
            dma((far - 1, share)),
            dma((nz, share)),
            dma((nz, share)),
        ],
        compiler_params=pltpu.CompilerParams(collective_id=1, has_side_effects=True, vmem_limit_bytes=62 * MIB),
    )(stat, num, hidden, w_o)


def solution(mesh):
    group = mesh.shape['sp']

    def local_step(hidden, w_norm, w_q, w_k, w_v, w_o, k_block, v_block, cache_len):
        q, k_new, v_new = project(hidden, w_norm, w_q, w_k, w_v, cache_len)
        k_out, v_out, num, stat = attend(q, k_new, v_new, k_block, v_block, cache_len)
        out = combine(num, stat, hidden, w_o, group)
        return out, k_out, v_out

    cache_spec = P('dp', 'sp', None)
    return jax.shard_map(local_step, mesh=mesh, in_specs=(P('dp', None), P(None), P(None, None), P(None, None), P(None, None), P(None, None), cache_spec, cache_spec, P('dp')), out_specs=(P('dp', None), cache_spec, cache_spec), check_vma=False)
```

```python
import functools

import jax
import jax.numpy as jnp
import numpy as np
from jax import lax
from jax.experimental import pallas as pl
from jax.experimental.pallas import tpu as pltpu
from jax.sharding import PartitionSpec as P

ROPE_BASE = 10000.0
EPSILON = 1e-6
MIB = 1024 * 1024
F32 = jnp.float32
BF16 = jnp.bfloat16
FLOOR = float(np.finfo(np.float32).min)
MESH = pl.DeviceIdType.MESH
TURN = (6.28125, 0.0019340515136718750, float(2 * np.pi - 6.28125 - 0.0019340515136718750))
ROW_BLOCK = 8
OUT_SLOTS = 12
OUT_TILE = 3072


def remote(src, dst, send_sem, recv_sem, device):
    return pltpu.make_async_remote_copy(src_ref=src, dst_ref=dst, send_sem=send_sem, recv_sem=recv_sem, device_id={'sp': device}, device_id_type=MESH)


def enter(devices):
    barrier = pltpu.get_barrier_semaphore()
    for device in devices:
        pl.semaphore_signal(barrier, inc=1, device_id={'sp': device}, device_id_type=MESH)
    pl.semaphore_wait(barrier, len(devices))


def project_kernel(freq_ref, len_ref, w_norm_ref, x_hbm, w_q_ref, w_k_ref, w_v_ref, q_ref, k_ref, v_ref, x_ref, x_norm, w_buf, q_buf, x_sem, w_sem, kv_sem, out_sem, send_sem, recv_sem):
    me = lax.axis_index('sp')
    core = me % 2
    partner = me + 1 - 2 * core
    num_rows, width = x_ref.shape
    head = k_ref.shape[1]
    half = q_ref.shape[1] // ROW_BLOCK // 2
    pair = 2 * head
    num_blocks = half // 2
    first_head = core * half

    def fetch(block):
        columns = pl.ds(pl.multiple_of((first_head + 2 * block) * head, pair), pair)
        return pltpu.make_async_copy(w_q_ref.at[:, columns], w_buf.at[block + 1], w_sem.at[block])

    fetch_k = pltpu.make_async_copy(w_k_ref, w_buf.at[0, :, pl.ds(0, head)], kv_sem.at[0])
    fetch_v = pltpu.make_async_copy(w_v_ref, w_buf.at[0, :, pl.ds(head, head)], kv_sem.at[1])
    fetch_x = pltpu.make_async_copy(x_hbm, x_ref, x_sem.at[0])
    fetch_x.start()
    fetch_k.start()
    fetch_v.start()
    for block in range(num_blocks):
        fetch(block).start()

    gain = 1.0 + w_norm_ref[...].astype(F32)
    angles = jnp.broadcast_to(len_ref[...].astype(F32), (num_rows, num_rows)).T * freq_ref[...]
    turns = jnp.round(angles * (0.5 / np.pi))
    for part in TURN:
        angles = angles - turns * part
    cos_t = jnp.cos(angles)
    sin_t = jnp.where(lax.broadcasted_iota(jnp.int32, angles.shape, 1) < head // 2, -1.0, 1.0) * jnp.sin(angles)
    fetch_x.wait()

    def normalise(step, carry):
        rows = pl.ds(pl.multiple_of(step * 16, 16), 16)
        x = x_ref[rows, :].astype(F32)
        inv_rms = lax.rsqrt(jnp.mean(x * x, axis=-1, keepdims=True) + EPSILON)
        x_norm[rows, :] = (x * inv_rms * gain).astype(BF16)
        return carry

    lax.fori_loop(0, num_rows // 16, normalise, 0)

    def rotate(u):
        u = u.astype(BF16).astype(F32)
        return u * cos_t + pltpu.roll(u, head // 2, 1) * sin_t

    fetch_k.wait()
    fetch_v.wait()
    both = jnp.dot(x_norm[...], w_buf[0], preferred_element_type=F32)
    k_ref[...] = rotate(both[:, :head]).astype(BF16).astype(F32)
    v_ref[...] = both[:, head:].astype(BF16).astype(F32)
    enter([partner])

    def heads_of(c, block):
        rows = pl.multiple_of((c * half + 2 * block) * ROW_BLOCK, 2 * ROW_BLOCK)
        return q_ref.at[:, pl.ds(rows, 2 * ROW_BLOCK), :]

    def keep(block):
        return pltpu.make_async_copy(q_buf.at[block], heads_of(core, block), out_sem.at[block])

    def send(block):
        return remote(q_buf.at[block], heads_of(core, block), send_sem.at[block], recv_sem.at[block], partner)

    def step(block, carry):
        fetch(block).wait()
        product = jnp.dot(x_norm[...], w_buf[block + 1], preferred_element_type=F32)
        for i in range(2):
            q = (rotate(product[:, i * head:(i + 1) * head]) * head ** -0.5).astype(BF16).astype(F32)
            q_buf[block, :, i * ROW_BLOCK:(i + 1) * ROW_BLOCK, :] = q.reshape(num_rows // ROW_BLOCK, ROW_BLOCK, head)
        send(block).start()
        keep(block).start()
        return carry

    lax.fori_loop(0, num_blocks, step, 0)

    def finish(block, carry):
        keep(block).wait()
        send(block).wait_send()
        other = heads_of(1 - core, block)
        remote(q_buf.at[block], other, send_sem.at[block], recv_sem.at[block], partner).wait_recv()
        return carry

    lax.fori_loop(0, num_blocks, finish, 0)


def project(hidden, w_norm, w_q, w_k, w_v, cache_len):
    num_rows, width = hidden.shape
    head = w_k.shape[1]
    heads = w_q.shape[1] // head
    inv_freq = ROPE_BASE ** (-np.arange(head // 2) * 2.0 / head)
    inv_freq = jnp.asarray(np.concatenate([inv_freq, inv_freq])[None, :], F32)
    vmem = pl.BlockSpec(memory_space=pltpu.VMEM)
    hbm = pl.BlockSpec(memory_space=pltpu.HBM)
    blocks = heads // 4
    return pl.pallas_call(
        project_kernel,
        name='project',
        out_shape=(jax.ShapeDtypeStruct((num_rows // ROW_BLOCK, heads * ROW_BLOCK, head), F32), jax.ShapeDtypeStruct((num_rows, head), F32), jax.ShapeDtypeStruct((num_rows, head), F32)),
        in_specs=[vmem, vmem, vmem, hbm, hbm, hbm, hbm],
        out_specs=(hbm, vmem, vmem),
        scratch_shapes=[
            pltpu.VMEM((num_rows, width), BF16),
            pltpu.VMEM((num_rows, width), BF16),
            pltpu.VMEM((blocks + 1, width, 2 * head), BF16),
            pltpu.VMEM((blocks, num_rows // ROW_BLOCK, 2 * ROW_BLOCK, head), F32),
            pltpu.SemaphoreType.DMA((1,)),
            pltpu.SemaphoreType.DMA((blocks,)),
            pltpu.SemaphoreType.DMA((2,)),
            pltpu.SemaphoreType.DMA((blocks,)),
            pltpu.SemaphoreType.DMA((blocks,)),
            pltpu.SemaphoreType.DMA((blocks,)),
        ],
        compiler_params=pltpu.CompilerParams(collective_id=0, has_side_effects=True, vmem_limit_bytes=60 * MIB),
    )(inv_freq, cache_len.reshape(1, -1), w_norm, hidden, w_q, w_k, w_v)


def attend_kernel(len_ref, k_new_ref, v_new_ref, q_hbm, k_hbm, v_hbm, k_out_hbm, v_out_hbm, num_hbm, stat_ref, q_ref, k_ref, v_ref, num_ref, scores_ref, in_sem, out_sem):
    num_rows, slots, head = k_ref.shape
    rows = ROW_BLOCK
    steps = num_rows // rows
    heads = stat_ref.shape[0] // 2
    base = lax.axis_index('sp') * slots
    group_iota = lax.broadcasted_iota(jnp.int32, (16, head), 0)
    lane_iota = lax.broadcasted_iota(jnp.int32, (heads, slots), 1)

    def loads(step):
        block = pl.ds(step * rows, rows)
        return [pltpu.make_async_copy(src, dst, in_sem.at[i, step]) for i, (src, dst) in enumerate(((k_hbm.at[block], k_ref.at[block]), (v_hbm.at[block], v_ref.at[block]), (q_hbm.at[step], q_ref.at[step])))]

    def stores(step):
        block = pl.ds(step * rows, rows)
        return [pltpu.make_async_copy(src, dst, out_sem.at[i, step]) for i, (src, dst) in enumerate(((k_ref.at[block], k_out_hbm.at[block]), (v_ref.at[block], v_out_hbm.at[block]), (num_ref.at[step], num_hbm.at[step])))]

    def start(step, carry):
        for copy in loads(step):
            copy.start()
        return carry

    def attend_rows(step, carry):
        first = step * rows
        for copy in loads(step):
            copy.wait()
        places = [len_ref[first + r] - base for r in range(rows)]
        for new, cache in ((k_new_ref, k_ref), (v_new_ref, v_ref)):
            fresh = new[pl.ds(pl.multiple_of(first, rows), rows), :]
            for r, p in enumerate(places):
                group = pl.multiple_of(jnp.clip(p, 0, slots - 1) // 16 * 16, 16)
                tile = cache[first + r, pl.ds(group, 16), :].astype(F32)
                cache[first + r, pl.ds(group, 16), :] = jnp.where(group_iota == p - group, fresh[r:r + 1, :], tile).astype(BF16)
        queries = q_ref.at[step]
        for r in range(rows):
            q = queries[pl.ds(r, heads, stride=rows), :].astype(BF16)
            scores_ref[r] = lax.dot_general(q, k_ref[first + r], (((1,), (1,)), ((), ())), preferred_element_type=F32)
        maxima, totals, factors = [], [], []
        for r, p in enumerate(places):
            valid = lane_iota <= p
            scores = jnp.where(valid, scores_ref[r], FLOOR)
            row_max = jnp.max(scores, axis=1, keepdims=True)
            weights = jnp.where(valid, jnp.exp(scores - row_max), 0.0)
            maxima.append(row_max)
            totals.append(jnp.sum(weights, axis=1, keepdims=True))
            factors.append(weights.astype(BF16))
        partial = num_ref.at[step]
        for r in range(rows):
            partial[pl.ds(r, heads, stride=rows), :] = jnp.dot(factors[r], v_ref[first + r], preferred_element_type=F32)
        stat_m = stat_ref[0:heads, :]
        stat_l = stat_ref[heads:2 * heads, :]
        for r in range(rows):
            here = lane_iota == first + r
            stat_m = jnp.where(here, maxima[r], stat_m)
            stat_l = jnp.where(here, totals[r], stat_l)
        stat_ref[0:heads, :] = stat_m
        stat_ref[heads:2 * heads, :] = stat_l
        for copy in stores(step):
            copy.start()
        return carry

    def finish(step, carry):
        for copy in stores(step):
            copy.wait()
        return carry

    lax.fori_loop(0, steps, start, 0)
    lax.fori_loop(0, steps, attend_rows, 0)
    lax.fori_loop(0, steps, finish, 0)


def attend(q, k_new, v_new, k_block, v_block, cache_len):
    num_rows, slots, head = k_block.shape
    steps = num_rows // ROW_BLOCK
    heads = q.shape[1] // ROW_BLOCK
    smem = pl.BlockSpec(memory_space=pltpu.SMEM)
    vmem = pl.BlockSpec(memory_space=pltpu.VMEM)
    hbm = pl.BlockSpec(memory_space=pltpu.HBM)
    return pl.pallas_call(
        attend_kernel,
        name='attend',
        out_shape=(jax.ShapeDtypeStruct(k_block.shape, BF16), jax.ShapeDtypeStruct(v_block.shape, BF16), jax.ShapeDtypeStruct(q.shape, F32), jax.ShapeDtypeStruct((2 * heads, num_rows), F32)),
        in_specs=[smem, vmem, vmem, hbm, hbm, hbm],
        out_specs=(hbm, hbm, hbm, vmem),
        scratch_shapes=[
            pltpu.VMEM(q.shape, F32),
            pltpu.VMEM(k_block.shape, BF16),
            pltpu.VMEM(v_block.shape, BF16),
            pltpu.VMEM(q.shape, F32),
            pltpu.VMEM((ROW_BLOCK, heads, slots), F32),
            pltpu.SemaphoreType.DMA((3, steps)),
            pltpu.SemaphoreType.DMA((3, steps)),
        ],
        compiler_params=pltpu.CompilerParams(vmem_limit_bytes=60 * MIB),
    )(cache_len, k_new, v_new, q, k_block, v_block)


def combine_kernel(nz, stat_ref, num_ref, x_hbm, w_o_ref, out_hbm, x_ref, out_ref, own_num, near_num, near_stat, part, from_long, from_short, gathered, total, attended, w_buf, x_sem, out_sem, own_sem, w_sem, stat_sem, near_send, near_recv, long_send, long_recv, short_send, short_recv, far_send, far_recv, back_send, back_recv, side_send, side_recv):
    me = lax.axis_index('sp')
    z = me // 2
    core = me % 2
    partner = me + 1 - 2 * core
    way = 1 - 2 * core
    num_rows, width = x_ref.shape
    heads = num_ref.shape[1] // ROW_BLOCK
    head = num_ref.shape[2]
    share = heads // (2 * nz)
    far = nz // 2

    def device(chip, c):
        return (chip + 2 * nz) % nz * 2 + c

    ahead = device(z + way, core)
    behind = device(z - way, core)
    targets = [far]
    for hop in range(far - 1, 0, -1):
        targets += [-hop, hop]
    targets.append(0)
    sources = [0]
    for hop in range(1, far):
        sources += [-hop, hop]
    sources.append(-far)

    units = [(0, s) for s in range(share)]
    for hop in range(1, far):
        units += [(sources.index(step), s) for s in range(share) for step in (-hop, hop)]
    units += [(nz - 1, s) for s in range(share)]

    def fetch(u):
        k, s = units[u]
        chip = z + way * sources[k]
        rows = [pl.ds(pl.multiple_of((device(chip, c) * share + s) * head, head), head) for c in range(2)]
        return [pltpu.make_async_copy(w_o_ref.at[rows[c], :], w_buf.at[u % OUT_SLOTS, c * head:(c + 1) * head, :], w_sem.at[u % OUT_SLOTS, c]) for c in range(2)]

    def start_fetch(u):
        for copy in fetch(u):
            copy.start()

    def own_heads(i, c):
        way_c = way * (1 - 2 * c)
        rows = share * ROW_BLOCK
        first = rows * device(z + way_c * targets[i], core + way * c)
        return num_ref.at[:, pl.ds(pl.multiple_of(first, rows), rows), :]

    own_copies = [pltpu.make_async_copy(own_heads(i, 0), own_num.at[i], own_sem.at[i]) for i in range(nz)]
    for copy in own_copies:
        copy.start()
    enter([partner, ahead, behind])
    swap_stat = remote(stat_ref, near_stat, stat_sem.at[0], stat_sem.at[1], partner)
    swap_stat.start()
    swaps = []
    for i in range(nz):
        swap = remote(own_heads(i, 1), near_num.at[i], near_send.at[i], near_recv.at[i], partner)
        swap.start()
        swaps.append(swap)
    fetch_x = pltpu.make_async_copy(x_hbm, x_ref, x_sem.at[0])
    fetch_x.start()
    for k in range(OUT_SLOTS):
        start_fetch(k)

    def column(row):
        return jnp.broadcast_to(row, (num_rows, num_rows)).T

    def merge(a, b):
        (x_a, m_a, l_a), (x_b, m_b, l_b) = a, b
        m = jnp.maximum(m_a, m_b)
        scale_a = jnp.exp(m_a - m)
        scale_b = jnp.exp(m_b - m)
        return x_a * column(scale_a) + x_b * column(scale_b), m, l_a * scale_a + l_b * scale_b

    def load(ref):
        return ref[0:num_rows, :], ref[num_rows:num_rows + 1, :], ref[num_rows + 1:num_rows + 2, :]

    sub_iota = lax.broadcasted_iota(jnp.int32, (8, num_rows), 0)

    def store(ref, triple):
        x, m, l = triple
        ref[0:num_rows, :] = x
        ref[num_rows:num_rows + 8, :] = jnp.where(sub_iota == 0, m, l)

    def own(i):
        own_copies[i].wait()
        swaps[i].wait_recv()
        first = share * device(z + way * targets[i], core)
        for s in range(share):
            h = first + s
            mine = (own_num[i, :, s * ROW_BLOCK:(s + 1) * ROW_BLOCK, :].reshape(num_rows, head), stat_ref[pl.ds(h, 1), :], stat_ref[pl.ds(heads + h, 1), :])
            theirs = (near_num[i, :, s * ROW_BLOCK:(s + 1) * ROW_BLOCK, :].reshape(num_rows, head), near_stat[pl.ds(h, 1), :], near_stat[pl.ds(heads + h, 1), :])
            store(part.at[i, s], merge(mine, theirs))

    def long_copy(hop, s):
        i = 0 if hop == 0 else 2 * hop
        return remote(part.at[i, s], from_long.at[hop, s], long_send.at[hop, s], long_recv.at[hop, s], ahead)

    def short_copy(hop, s):
        return remote(part.at[2 * hop + 1, s], from_short.at[hop, s], short_send.at[hop, s], short_recv.at[hop, s], behind)

    swap_stat.wait_recv()
    for hop in range(far):
        own(2 * hop)
        if hop == 0:
            for s in range(share):
                long_copy(0, s).start()
        own(2 * hop + 1)
        if hop == 0:
            for s in range(share):
                short_copy(0, s).start()
            continue
        for s in range(share):
            long_copy(hop - 1, s).wait_recv()
            store(part.at[2 * hop, s], merge(load(part.at[2 * hop, s]), load(from_long.at[hop - 1, s])))
            long_copy(hop, s).start()
            if hop < far - 1:
                short_copy(hop - 1, s).wait_recv()
                store(part.at[2 * hop + 1, s], merge(load(part.at[2 * hop + 1, s]), load(from_short.at[hop - 1, s])))
                short_copy(hop, s).start()

    def far_copy(hop, s):
        slot = gathered.at[device(z - way * hop, core), s]
        return remote(slot, slot, far_send.at[hop, s], far_recv.at[hop, s], ahead)

    def back_copy(hop, s):
        slot = gathered.at[device(z + way * hop, core), s]
        return remote(slot, slot, back_send.at[hop, s], back_recv.at[hop, s], behind)

    def side_copy(k, s):
        slot = gathered.at[device(z + way * sources[k], core), s]
        return remote(slot, slot, side_send.at[k, s], side_recv.at[k, s], partner)

    def far_arrival(hop, s):
        slot = gathered.at[device(z - way * (hop + 1), core), s]
        return remote(slot, slot, far_send.at[hop, s], far_recv.at[hop, s], ahead)

    def back_arrival(hop, s):
        slot = gathered.at[device(z + way * (hop + 1), core), s]
        return remote(slot, slot, back_send.at[hop, s], back_recv.at[hop, s], behind)

    def side_arrival(k, s):
        slot = gathered.at[device(z - way * sources[k], 1 - core), s]
        return remote(slot, slot, side_send.at[k, s], side_recv.at[k, s], partner)

    mirror = {hop: k for k, hop in enumerate(sources)}
    mirror[far] = mirror[-far]

    last = far - 1
    for s in range(share):
        short_copy(last - 1, s).wait_recv()
        triple = merge(load(part.at[2 * far - 1, s]), load(from_short.at[last - 1, s]))
        long_copy(last, s).wait_recv()
        x, _, l = merge(triple, load(from_long.at[last, s]))
        gathered[me, s] = (x / column(l)).astype(BF16).astype(F32)
        far_copy(0, s).start()
        back_copy(0, s).start()
        side_copy(0, s).start()

    tiles = width // OUT_TILE

    def save(n):
        columns = pl.ds(pl.multiple_of(n * OUT_TILE, OUT_TILE), OUT_TILE)
        return pltpu.make_async_copy(out_ref.at[:, columns], out_hbm.at[:, columns], out_sem.at[n])

    def multiply(us):
        for i, u in enumerate(us):
            k, s = units[u]
            side_arrival(mirror[-sources[k]], s).wait_recv()
            chip = z + way * sources[k]
            for c in range(2):
                attended[i, :, c * head:(c + 1) * head] = gathered[device(chip, c), s].astype(BF16)
            for copy in fetch(u):
                copy.wait()

        def tile(n, carry):
            columns = pl.ds(pl.multiple_of(n * OUT_TILE, OUT_TILE), OUT_TILE)
            product = None
            for i, u in enumerate(us):
                term = jnp.dot(attended[i], w_buf[u % OUT_SLOTS, :, columns], preferred_element_type=F32)
                product = term if product is None else product + term
            before = x_ref[:, columns].astype(F32) if 0 in us else total[:, columns]
            if len(units) - 1 in us:
                out_ref[:, columns] = (before + product).astype(BF16)
                save(n).start()
            else:
                total[:, columns] = before + product
            return carry

        lax.fori_loop(0, tiles, tile, 0)
        for u in us:
            if u + OUT_SLOTS < len(units):
                start_fetch(u + OUT_SLOTS)

    chunks = [[s] for s in range(share)]
    while sum(map(len, chunks)) < len(units) - share:
        u = sum(map(len, chunks))
        chunks.append([u, u + 1])
    chunks += [[len(units) - share + s] for s in range(share)]
    fetch_x.wait()
    multiply(chunks.pop(0))
    multiply(chunks.pop(0))
    for hop in range(far):
        for s in range(share):
            far_arrival(hop, s).wait_recv()
            if hop < far - 1:
                far_copy(hop + 1, s).start()
            side_copy(mirror[-(hop + 1)], s).start()
            if hop < far - 1:
                back_arrival(hop, s).wait_recv()
                if hop < far - 2:
                    back_copy(hop + 1, s).start()
                side_copy(mirror[hop + 1], s).start()
            multiply(chunks.pop(0))
    for chunk in chunks:
        multiply(chunk)
    for n in range(tiles):
        save(n).wait()

    swap_stat.wait_send()
    for swap in swaps:
        swap.wait_send()
    for s in range(share):
        for hop in range(far):
            long_copy(hop, s).wait_send()
            far_copy(hop, s).wait_send()
            if hop < far - 1:
                short_copy(hop, s).wait_send()
                back_copy(hop, s).wait_send()
        for k in range(nz):
            side_copy(k, s).wait_send()


def combine(num, stat, hidden, w_o, group):
    num_rows, width = hidden.shape
    heads = num.shape[1] // ROW_BLOCK
    head = num.shape[2]
    nz = group // 2
    share = heads // group
    far = nz // 2
    vmem = pl.BlockSpec(memory_space=pltpu.VMEM)
    hbm = pl.BlockSpec(memory_space=pltpu.HBM)
    dma = pltpu.SemaphoreType.DMA
    piece = (num_rows + 8, head)
    return pl.pallas_call(
        functools.partial(combine_kernel, nz),
        name='combine',
        out_shape=jax.ShapeDtypeStruct((num_rows, width), BF16),
        in_specs=[vmem, hbm, hbm, hbm],
        out_specs=hbm,
        scratch_shapes=[
            pltpu.VMEM((num_rows, width), BF16),
            pltpu.VMEM((num_rows, width), BF16),
            pltpu.VMEM((nz, num_rows // ROW_BLOCK, share * ROW_BLOCK, head), F32),
            pltpu.VMEM((nz, num_rows // ROW_BLOCK, share * ROW_BLOCK, head), F32),
            pltpu.VMEM((2 * heads, num_rows), F32),
            pltpu.VMEM((nz, share) + piece, F32),
            pltpu.VMEM((far, share) + piece, F32),
            pltpu.VMEM((far - 1, share) + piece, F32),
            pltpu.VMEM((group, share, num_rows, head), F32),
            pltpu.VMEM((num_rows, width), F32),
            pltpu.VMEM((2, num_rows, 2 * head), BF16),
            pltpu.VMEM((OUT_SLOTS, 2 * head, width), BF16),
            dma((1,)),
            dma((width // OUT_TILE,)),
            dma((nz,)),
            dma((OUT_SLOTS, 2)),
            dma((2,)),
            dma((nz,)),
            dma((nz,)),
            dma((far, share)),
            dma((far, share)),
            dma((far - 1, share)),
            dma((far - 1, share)),
            dma((far, share)),
            dma((far, share)),
            dma((far - 1, share)),
            dma((far - 1, share)),
            dma((nz, share)),
            dma((nz, share)),
        ],
        compiler_params=pltpu.CompilerParams(collective_id=1, has_side_effects=True, vmem_limit_bytes=62 * MIB),
    )(stat, num, hidden, w_o)


def solution(mesh):
    group = mesh.shape['sp']

    def local_step(hidden, w_norm, w_q, w_k, w_v, w_o, k_block, v_block, cache_len):
        q, k_new, v_new = project(hidden, w_norm, w_q, w_k, w_v, cache_len)
        k_out, v_out, num, stat = attend(q, k_new, v_new, k_block, v_block, cache_len)
        out = combine(num, stat, hidden, w_o, group)
        return out, k_out, v_out

    cache_spec = P('dp', 'sp', None)
    return jax.shard_map(local_step, mesh=mesh, in_specs=(P('dp', None), P(None), P(None, None), P(None, None), P(None, None), P(None, None), cache_spec, cache_spec, P('dp')), out_specs=(P('dp', None), cache_spec, cache_spec), check_vma=False)
```

```python
import functools

import jax
import jax.numpy as jnp
import numpy as np
from jax import lax
from jax.experimental import pallas as pl
from jax.experimental.pallas import tpu as pltpu
from jax.sharding import PartitionSpec as P

ROPE_BASE = 10000.0
EPSILON = 1e-6
MIB = 1024 * 1024
F32 = jnp.float32
BF16 = jnp.bfloat16
FLOOR = float(np.finfo(np.float32).min)
MESH = pl.DeviceIdType.MESH
TURN = (6.28125, 0.0019340515136718750, float(2 * np.pi - 6.28125 - 0.0019340515136718750))
ROW_BLOCK = 8
OUT_SLOTS = 12
PROJ_WINDOW = 4
ATTEND_WINDOW = 4
OUT_TILE = 3072


def remote(src, dst, send_sem, recv_sem, device):
    return pltpu.make_async_remote_copy(src_ref=src, dst_ref=dst, send_sem=send_sem, recv_sem=recv_sem, device_id={'sp': device}, device_id_type=MESH)


def enter(devices):
    barrier = pltpu.get_barrier_semaphore()
    for device in devices:
        pl.semaphore_signal(barrier, inc=1, device_id={'sp': device}, device_id_type=MESH)
    pl.semaphore_wait(barrier, len(devices))


def project_kernel(freq_ref, len_ref, w_norm_ref, x_hbm, w_q_ref, w_k_ref, w_v_ref, q_ref, k_ref, v_ref, x_ref, x_norm, w_buf, q_buf, x_sem, w_sem, kv_sem, out_sem, send_sem, recv_sem):
    me = lax.axis_index('sp')
    core = me % 2
    partner = me + 1 - 2 * core
    num_rows, width = x_ref.shape
    head = k_ref.shape[1]
    half = q_ref.shape[1] // ROW_BLOCK // 2
    pair = 2 * head
    num_blocks = half // 2
    first_head = core * half

    def fetch(block):
        columns = pl.ds(pl.multiple_of((first_head + 2 * block) * head, pair), pair)
        return pltpu.make_async_copy(w_q_ref.at[:, columns], w_buf.at[block + 1], w_sem.at[block])

    fetch_k = pltpu.make_async_copy(w_k_ref, w_buf.at[0, :, pl.ds(0, head)], kv_sem.at[0])
    fetch_v = pltpu.make_async_copy(w_v_ref, w_buf.at[0, :, pl.ds(head, head)], kv_sem.at[1])
    fetch_x = pltpu.make_async_copy(x_hbm, x_ref, x_sem.at[0])
    fetch_x.start()
    fetch_k.start()
    fetch_v.start()
    fetch(0).start()

    gain = 1.0 + w_norm_ref[...].astype(F32)
    angles = jnp.broadcast_to(len_ref[...].astype(F32), (num_rows, num_rows)).T * freq_ref[...]
    turns = jnp.round(angles * (0.5 / np.pi))
    for part in TURN:
        angles = angles - turns * part
    cos_t = jnp.cos(angles)
    sin_t = jnp.where(lax.broadcasted_iota(jnp.int32, angles.shape, 1) < head // 2, -1.0, 1.0) * jnp.sin(angles)
    fetch_x.wait()
    for block in range(1, PROJ_WINDOW):
        fetch(block).start()

    def normalise(step, carry):
        rows = pl.ds(pl.multiple_of(step * 16, 16), 16)
        x = x_ref[rows, :].astype(F32)
        inv_rms = lax.rsqrt(jnp.mean(x * x, axis=-1, keepdims=True) + EPSILON)
        x_norm[rows, :] = (x * inv_rms * gain).astype(BF16)
        return carry

    lax.fori_loop(0, num_rows // 16, normalise, 0)

    def rotate(u):
        u = u.astype(BF16).astype(F32)
        return u * cos_t + pltpu.roll(u, head // 2, 1) * sin_t

    fetch_k.wait()
    fetch_v.wait()
    both = jnp.dot(x_norm[...], w_buf[0], preferred_element_type=F32)
    k_ref[...] = rotate(both[:, :head]).astype(BF16).astype(F32)
    v_ref[...] = both[:, head:].astype(BF16).astype(F32)
    enter([partner])

    def heads_of(c, block):
        rows = pl.multiple_of((c * half + 2 * block) * ROW_BLOCK, 2 * ROW_BLOCK)
        return q_ref.at[:, pl.ds(rows, 2 * ROW_BLOCK), :]

    def keep(block):
        return pltpu.make_async_copy(q_buf.at[block], heads_of(core, block), out_sem.at[block])

    def send(block):
        return remote(q_buf.at[block], heads_of(core, block), send_sem.at[block], recv_sem.at[block], partner)

    def step(block, carry):
        @pl.when(block + PROJ_WINDOW < num_blocks)
        def _():
            fetch(block + PROJ_WINDOW).start()

        fetch(block).wait()
        product = jnp.dot(x_norm[...], w_buf[block + 1], preferred_element_type=F32)
        for i in range(2):
            q = (rotate(product[:, i * head:(i + 1) * head]) * head ** -0.5).astype(BF16).astype(F32)
            q_buf[block, :, i * ROW_BLOCK:(i + 1) * ROW_BLOCK, :] = q.reshape(num_rows // ROW_BLOCK, ROW_BLOCK, head)
        send(block).start()
        keep(block).start()
        return carry

    lax.fori_loop(0, num_blocks, step, 0)

    def finish(block, carry):
        keep(block).wait()
        send(block).wait_send()
        other = heads_of(1 - core, block)
        remote(q_buf.at[block], other, send_sem.at[block], recv_sem.at[block], partner).wait_recv()
        return carry

    lax.fori_loop(0, num_blocks, finish, 0)


def project(hidden, w_norm, w_q, w_k, w_v, cache_len):
    num_rows, width = hidden.shape
    head = w_k.shape[1]
    heads = w_q.shape[1] // head
    inv_freq = ROPE_BASE ** (-np.arange(head // 2) * 2.0 / head)
    inv_freq = jnp.asarray(np.concatenate([inv_freq, inv_freq])[None, :], F32)
    vmem = pl.BlockSpec(memory_space=pltpu.VMEM)
    hbm = pl.BlockSpec(memory_space=pltpu.HBM)
    blocks = heads // 4
    return pl.pallas_call(
        project_kernel,
        name='project',
        out_shape=(jax.ShapeDtypeStruct((num_rows // ROW_BLOCK, heads * ROW_BLOCK, head), F32), jax.ShapeDtypeStruct((num_rows, head), F32), jax.ShapeDtypeStruct((num_rows, head), F32)),
        in_specs=[vmem, vmem, vmem, hbm, hbm, hbm, hbm],
        out_specs=(hbm, vmem, vmem),
        scratch_shapes=[
            pltpu.VMEM((num_rows, width), BF16),
            pltpu.VMEM((num_rows, width), BF16),
            pltpu.VMEM((blocks + 1, width, 2 * head), BF16),
            pltpu.VMEM((blocks, num_rows // ROW_BLOCK, 2 * ROW_BLOCK, head), F32),
            pltpu.SemaphoreType.DMA((1,)),
            pltpu.SemaphoreType.DMA((blocks,)),
            pltpu.SemaphoreType.DMA((2,)),
            pltpu.SemaphoreType.DMA((blocks,)),
            pltpu.SemaphoreType.DMA((blocks,)),
            pltpu.SemaphoreType.DMA((blocks,)),
        ],
        compiler_params=pltpu.CompilerParams(collective_id=0, has_side_effects=True, vmem_limit_bytes=60 * MIB),
    )(inv_freq, cache_len.reshape(1, -1), w_norm, hidden, w_q, w_k, w_v)


def attend_kernel(len_ref, k_new_ref, v_new_ref, q_hbm, k_hbm, v_hbm, k_out_hbm, v_out_hbm, num_hbm, stat_ref, q_ref, k_ref, v_ref, num_ref, scores_ref, in_sem, out_sem):
    num_rows, slots, head = k_ref.shape
    rows = ROW_BLOCK
    steps = num_rows // rows
    heads = stat_ref.shape[0] // 2
    base = lax.axis_index('sp') * slots
    group_iota = lax.broadcasted_iota(jnp.int32, (16, head), 0)
    lane_iota = lax.broadcasted_iota(jnp.int32, (heads, slots), 1)

    def loads(step):
        block = pl.ds(step * rows, rows)
        return [pltpu.make_async_copy(src, dst, in_sem.at[i, step]) for i, (src, dst) in enumerate(((k_hbm.at[block], k_ref.at[block]), (v_hbm.at[block], v_ref.at[block]), (q_hbm.at[step], q_ref.at[step])))]

    def stores(step):
        block = pl.ds(step * rows, rows)
        return [pltpu.make_async_copy(src, dst, out_sem.at[i, step]) for i, (src, dst) in enumerate(((k_ref.at[block], k_out_hbm.at[block]), (v_ref.at[block], v_out_hbm.at[block]), (num_ref.at[step], num_hbm.at[step])))]

    def start(step, carry):
        for copy in loads(step):
            copy.start()
        return carry

    def attend_rows(step, carry):
        first = step * rows

        @pl.when(step + ATTEND_WINDOW < steps)
        def _():
            start(step + ATTEND_WINDOW, 0)

        for copy in loads(step):
            copy.wait()
        places = [len_ref[first + r] - base for r in range(rows)]
        for new, cache in ((k_new_ref, k_ref), (v_new_ref, v_ref)):
            fresh = new[pl.ds(pl.multiple_of(first, rows), rows), :]
            for r, p in enumerate(places):
                group = pl.multiple_of(jnp.clip(p, 0, slots - 1) // 16 * 16, 16)
                tile = cache[first + r, pl.ds(group, 16), :].astype(F32)
                cache[first + r, pl.ds(group, 16), :] = jnp.where(group_iota == p - group, fresh[r:r + 1, :], tile).astype(BF16)
        queries = q_ref.at[step]
        for r in range(rows):
            q = queries[pl.ds(r, heads, stride=rows), :].astype(BF16)
            scores_ref[r] = lax.dot_general(q, k_ref[first + r], (((1,), (1,)), ((), ())), preferred_element_type=F32)
        maxima, totals, factors = [], [], []
        for r, p in enumerate(places):
            valid = lane_iota <= p
            scores = jnp.where(valid, scores_ref[r], FLOOR)
            row_max = jnp.max(scores, axis=1, keepdims=True)
            weights = jnp.where(valid, jnp.exp(scores - row_max), 0.0)
            maxima.append(row_max)
            totals.append(jnp.sum(weights, axis=1, keepdims=True))
            factors.append(weights.astype(BF16))
        partial = num_ref.at[step]
        for r in range(rows):
            partial[pl.ds(r, heads, stride=rows), :] = jnp.dot(factors[r], v_ref[first + r], preferred_element_type=F32)
        stat_m = stat_ref[0:heads, :]
        stat_l = stat_ref[heads:2 * heads, :]
        for r in range(rows):
            here = lane_iota == first + r
            stat_m = jnp.where(here, maxima[r], stat_m)
            stat_l = jnp.where(here, totals[r], stat_l)
        stat_ref[0:heads, :] = stat_m
        stat_ref[heads:2 * heads, :] = stat_l
        for copy in stores(step):
            copy.start()
        return carry

    def finish(step, carry):
        for copy in stores(step):
            copy.wait()
        return carry

    lax.fori_loop(0, ATTEND_WINDOW, start, 0)
    lax.fori_loop(0, steps, attend_rows, 0)
    lax.fori_loop(0, steps, finish, 0)


def attend(q, k_new, v_new, k_block, v_block, cache_len):
    num_rows, slots, head = k_block.shape
    steps = num_rows // ROW_BLOCK
    heads = q.shape[1] // ROW_BLOCK
    smem = pl.BlockSpec(memory_space=pltpu.SMEM)
    vmem = pl.BlockSpec(memory_space=pltpu.VMEM)
    hbm = pl.BlockSpec(memory_space=pltpu.HBM)
    return pl.pallas_call(
        attend_kernel,
        name='attend',
        out_shape=(jax.ShapeDtypeStruct(k_block.shape, BF16), jax.ShapeDtypeStruct(v_block.shape, BF16), jax.ShapeDtypeStruct(q.shape, F32), jax.ShapeDtypeStruct((2 * heads, num_rows), F32)),
        in_specs=[smem, vmem, vmem, hbm, hbm, hbm],
        out_specs=(hbm, hbm, hbm, vmem),
        scratch_shapes=[
            pltpu.VMEM(q.shape, F32),
            pltpu.VMEM(k_block.shape, BF16),
            pltpu.VMEM(v_block.shape, BF16),
            pltpu.VMEM(q.shape, F32),
            pltpu.VMEM((ROW_BLOCK, heads, slots), F32),
            pltpu.SemaphoreType.DMA((3, steps)),
            pltpu.SemaphoreType.DMA((3, steps)),
        ],
        compiler_params=pltpu.CompilerParams(vmem_limit_bytes=60 * MIB),
    )(cache_len, k_new, v_new, q, k_block, v_block)


def combine_kernel(nz, stat_ref, num_ref, x_hbm, w_o_ref, out_hbm, x_ref, out_ref, own_num, near_num, near_stat, part, from_long, from_short, gathered, total, attended, w_buf, x_sem, out_sem, own_sem, w_sem, stat_sem, near_send, near_recv, long_send, long_recv, short_send, short_recv, far_send, far_recv, back_send, back_recv, side_send, side_recv):
    me = lax.axis_index('sp')
    z = me // 2
    core = me % 2
    partner = me + 1 - 2 * core
    way = 1 - 2 * core
    num_rows, width = x_ref.shape
    heads = num_ref.shape[1] // ROW_BLOCK
    head = num_ref.shape[2]
    share = heads // (2 * nz)
    far = nz // 2

    def device(chip, c):
        return (chip + 2 * nz) % nz * 2 + c

    ahead = device(z + way, core)
    behind = device(z - way, core)
    targets = [far]
    for hop in range(far - 1, 0, -1):
        targets += [-hop, hop]
    targets.append(0)
    sources = [0]
    for hop in range(1, far):
        sources += [-hop, hop]
    sources.append(-far)

    units = [(0, s) for s in range(share)]
    for hop in range(1, far):
        units += [(sources.index(step), s) for s in range(share) for step in (-hop, hop)]
    units += [(nz - 1, s) for s in range(share)]

    def fetch(u):
        k, s = units[u]
        chip = z + way * sources[k]
        rows = [pl.ds(pl.multiple_of((device(chip, c) * share + s) * head, head), head) for c in range(2)]
        return [pltpu.make_async_copy(w_o_ref.at[rows[c], :], w_buf.at[u % OUT_SLOTS, c * head:(c + 1) * head, :], w_sem.at[u % OUT_SLOTS, c]) for c in range(2)]

    def start_fetch(u):
        for copy in fetch(u):
            copy.start()

    def own_heads(i, c):
        way_c = way * (1 - 2 * c)
        rows = share * ROW_BLOCK
        first = rows * device(z + way_c * targets[i], core + way * c)
        return num_ref.at[:, pl.ds(pl.multiple_of(first, rows), rows), :]

    own_copies = [pltpu.make_async_copy(own_heads(i, 0), own_num.at[i], own_sem.at[i]) for i in range(nz)]
    for copy in own_copies:
        copy.start()
    enter([partner, ahead, behind])
    swap_stat = remote(stat_ref, near_stat, stat_sem.at[0], stat_sem.at[1], partner)
    swap_stat.start()
    swaps = []
    for i in range(nz):
        swap = remote(own_heads(i, 1), near_num.at[i], near_send.at[i], near_recv.at[i], partner)
        swap.start()
        swaps.append(swap)
    fetch_x = pltpu.make_async_copy(x_hbm, x_ref, x_sem.at[0])
    ahead_of_use = list(range(OUT_SLOTS))

    def fetch_some(count):
        for _ in range(count):
            if ahead_of_use:
                start_fetch(ahead_of_use.pop(0))

    def column(row):
        return jnp.broadcast_to(row, (num_rows, num_rows)).T

    def merge(a, b):
        (x_a, m_a, l_a), (x_b, m_b, l_b) = a, b
        m = jnp.maximum(m_a, m_b)
        scale_a = jnp.exp(m_a - m)
        scale_b = jnp.exp(m_b - m)
        return x_a * column(scale_a) + x_b * column(scale_b), m, l_a * scale_a + l_b * scale_b

    def load(ref):
        return ref[0:num_rows, :], ref[num_rows:num_rows + 1, :], ref[num_rows + 1:num_rows + 2, :]

    sub_iota = lax.broadcasted_iota(jnp.int32, (8, num_rows), 0)

    def store(ref, triple):
        x, m, l = triple
        ref[0:num_rows, :] = x
        ref[num_rows:num_rows + 8, :] = jnp.where(sub_iota == 0, m, l)

    def own(i):
        own_copies[i].wait()
        swaps[i].wait_recv()
        first = share * device(z + way * targets[i], core)
        for s in range(share):
            h = first + s
            mine = (own_num[i, :, s * ROW_BLOCK:(s + 1) * ROW_BLOCK, :].reshape(num_rows, head), stat_ref[pl.ds(h, 1), :], stat_ref[pl.ds(heads + h, 1), :])
            theirs = (near_num[i, :, s * ROW_BLOCK:(s + 1) * ROW_BLOCK, :].reshape(num_rows, head), near_stat[pl.ds(h, 1), :], near_stat[pl.ds(heads + h, 1), :])
            store(part.at[i, s], merge(mine, theirs))

    def long_copy(hop, s):
        i = 0 if hop == 0 else 2 * hop
        return remote(part.at[i, s], from_long.at[hop, s], long_send.at[hop, s], long_recv.at[hop, s], ahead)

    def short_copy(hop, s):
        return remote(part.at[2 * hop + 1, s], from_short.at[hop, s], short_send.at[hop, s], short_recv.at[hop, s], behind)

    swap_stat.wait_recv()
    for hop in range(far):
        own(2 * hop)
        if hop == 0:
            for s in range(share):
                long_copy(0, s).start()
        own(2 * hop + 1)
        if hop == 0:
            for s in range(share):
                short_copy(0, s).start()
            fetch_x.start()
            fetch_some(2)
            continue
        for s in range(share):
            long_copy(hop - 1, s).wait_recv()
            store(part.at[2 * hop, s], merge(load(part.at[2 * hop, s]), load(from_long.at[hop - 1, s])))
            long_copy(hop, s).start()
            fetch_some(2)
            if hop < far - 1:
                short_copy(hop - 1, s).wait_recv()
                store(part.at[2 * hop + 1, s], merge(load(part.at[2 * hop + 1, s]), load(from_short.at[hop - 1, s])))
                short_copy(hop, s).start()

    def far_copy(hop, s):
        slot = gathered.at[device(z - way * hop, core), s]
        return remote(slot, slot, far_send.at[hop, s], far_recv.at[hop, s], ahead)

    def back_copy(hop, s):
        slot = gathered.at[device(z + way * hop, core), s]
        return remote(slot, slot, back_send.at[hop, s], back_recv.at[hop, s], behind)

    def side_copy(k, s):
        slot = gathered.at[device(z + way * sources[k], core), s]
        return remote(slot, slot, side_send.at[k, s], side_recv.at[k, s], partner)

    def far_arrival(hop, s):
        slot = gathered.at[device(z - way * (hop + 1), core), s]
        return remote(slot, slot, far_send.at[hop, s], far_recv.at[hop, s], ahead)

    def back_arrival(hop, s):
        slot = gathered.at[device(z + way * (hop + 1), core), s]
        return remote(slot, slot, back_send.at[hop, s], back_recv.at[hop, s], behind)

    def side_arrival(k, s):
        slot = gathered.at[device(z - way * sources[k], 1 - core), s]
        return remote(slot, slot, side_send.at[k, s], side_recv.at[k, s], partner)

    mirror = {hop: k for k, hop in enumerate(sources)}
    mirror[far] = mirror[-far]

    last = far - 1
    fetch_some(OUT_SLOTS)
    for s in range(share):
        short_copy(last - 1, s).wait_recv()
        triple = merge(load(part.at[2 * far - 1, s]), load(from_short.at[last - 1, s]))
        long_copy(last, s).wait_recv()
        x, _, l = merge(triple, load(from_long.at[last, s]))
        gathered[me, s] = (x / column(l)).astype(BF16).astype(F32)
        far_copy(0, s).start()
        back_copy(0, s).start()
        side_copy(0, s).start()

    tiles = width // OUT_TILE

    def save(n):
        columns = pl.ds(pl.multiple_of(n * OUT_TILE, OUT_TILE), OUT_TILE)
        return pltpu.make_async_copy(out_ref.at[:, columns], out_hbm.at[:, columns], out_sem.at[n])

    def multiply(us):
        for i, u in enumerate(us):
            k, s = units[u]
            side_arrival(mirror[-sources[k]], s).wait_recv()
            chip = z + way * sources[k]
            for c in range(2):
                attended[i, :, c * head:(c + 1) * head] = gathered[device(chip, c), s].astype(BF16)
            for copy in fetch(u):
                copy.wait()

        def tile(n, carry):
            columns = pl.ds(pl.multiple_of(n * OUT_TILE, OUT_TILE), OUT_TILE)
            product = None
            for i, u in enumerate(us):
                term = jnp.dot(attended[i], w_buf[u % OUT_SLOTS, :, columns], preferred_element_type=F32)
                product = term if product is None else product + term
            before = x_ref[:, columns].astype(F32) if 0 in us else total[:, columns]
            if len(units) - 1 in us:
                out_ref[:, columns] = (before + product).astype(BF16)
                save(n).start()
            else:
                total[:, columns] = before + product
            return carry

        lax.fori_loop(0, tiles, tile, 0)
        for u in us:
            if u + OUT_SLOTS < len(units):
                start_fetch(u + OUT_SLOTS)

    chunks = [[s] for s in range(share)]
    while sum(map(len, chunks)) < len(units) - share:
        u = sum(map(len, chunks))
        chunks.append([u, u + 1])
    chunks += [[len(units) - share + s] for s in range(share)]
    fetch_x.wait()
    multiply(chunks.pop(0))
    multiply(chunks.pop(0))
    for hop in range(far):
        for s in range(share):
            far_arrival(hop, s).wait_recv()
            if hop < far - 1:
                far_copy(hop + 1, s).start()
            side_copy(mirror[-(hop + 1)], s).start()
            if hop < far - 1:
                back_arrival(hop, s).wait_recv()
                if hop < far - 2:
                    back_copy(hop + 1, s).start()
                side_copy(mirror[hop + 1], s).start()
            multiply(chunks.pop(0))
    for chunk in chunks:
        multiply(chunk)
    for n in range(tiles):
        save(n).wait()

    swap_stat.wait_send()
    for swap in swaps:
        swap.wait_send()
    for s in range(share):
        for hop in range(far):
            long_copy(hop, s).wait_send()
            far_copy(hop, s).wait_send()
            if hop < far - 1:
                short_copy(hop, s).wait_send()
                back_copy(hop, s).wait_send()
        for k in range(nz):
            side_copy(k, s).wait_send()


def combine(num, stat, hidden, w_o, group):
    num_rows, width = hidden.shape
    heads = num.shape[1] // ROW_BLOCK
    head = num.shape[2]
    nz = group // 2
    share = heads // group
    far = nz // 2
    vmem = pl.BlockSpec(memory_space=pltpu.VMEM)
    hbm = pl.BlockSpec(memory_space=pltpu.HBM)
    dma = pltpu.SemaphoreType.DMA
    piece = (num_rows + 8, head)
    return pl.pallas_call(
        functools.partial(combine_kernel, nz),
        name='combine',
        out_shape=jax.ShapeDtypeStruct((num_rows, width), BF16),
        in_specs=[vmem, hbm, hbm, hbm],
        out_specs=hbm,
        scratch_shapes=[
            pltpu.VMEM((num_rows, width), BF16),
            pltpu.VMEM((num_rows, width), BF16),
            pltpu.VMEM((nz, num_rows // ROW_BLOCK, share * ROW_BLOCK, head), F32),
            pltpu.VMEM((nz, num_rows // ROW_BLOCK, share * ROW_BLOCK, head), F32),
            pltpu.VMEM((2 * heads, num_rows), F32),
            pltpu.VMEM((nz, share) + piece, F32),
            pltpu.VMEM((far, share) + piece, F32),
            pltpu.VMEM((far - 1, share) + piece, F32),
            pltpu.VMEM((group, share, num_rows, head), F32),
            pltpu.VMEM((num_rows, width), F32),
            pltpu.VMEM((2, num_rows, 2 * head), BF16),
            pltpu.VMEM((OUT_SLOTS, 2 * head, width), BF16),
            dma((1,)),
            dma((width // OUT_TILE,)),
            dma((nz,)),
            dma((OUT_SLOTS, 2)),
            dma((2,)),
            dma((nz,)),
            dma((nz,)),
            dma((far, share)),
            dma((far, share)),
            dma((far - 1, share)),
            dma((far - 1, share)),
            dma((far, share)),
            dma((far, share)),
            dma((far - 1, share)),
            dma((far - 1, share)),
            dma((nz, share)),
            dma((nz, share)),
        ],
        compiler_params=pltpu.CompilerParams(collective_id=1, has_side_effects=True, vmem_limit_bytes=62 * MIB),
    )(stat, num, hidden, w_o)


def solution(mesh):
    group = mesh.shape['sp']

    def local_step(hidden, w_norm, w_q, w_k, w_v, w_o, k_block, v_block, cache_len):
        q, k_new, v_new = project(hidden, w_norm, w_q, w_k, w_v, cache_len)
        k_out, v_out, num, stat = attend(q, k_new, v_new, k_block, v_block, cache_len)
        out = combine(num, stat, hidden, w_o, group)
        return out, k_out, v_out

    cache_spec = P('dp', 'sp', None)
    return jax.shard_map(local_step, mesh=mesh, in_specs=(P('dp', None), P(None), P(None, None), P(None, None), P(None, None), P(None, None), cache_spec, cache_spec, P('dp')), out_specs=(P('dp', None), cache_spec, cache_spec), check_vma=False)
```

```python
import functools

import jax
import jax.numpy as jnp
import numpy as np
from jax import lax
from jax.experimental import pallas as pl
from jax.experimental.pallas import tpu as pltpu
from jax.sharding import PartitionSpec as P

ROPE_BASE = 10000.0
EPSILON = 1e-6
MIB = 1024 * 1024
F32 = jnp.float32
BF16 = jnp.bfloat16
FLOOR = float(np.finfo(np.float32).min)
MESH = pl.DeviceIdType.MESH
TURN = (6.28125, 0.0019340515136718750, float(2 * np.pi - 6.28125 - 0.0019340515136718750))
ROW_BLOCK = 8
OUT_SLOTS = 12
PROJ_WINDOW = 4
ATTEND_WINDOW = 3
ATTEND_BLOCKS = 2
OUT_TILE = 3072


def remote(src, dst, send_sem, recv_sem, device):
    return pltpu.make_async_remote_copy(src_ref=src, dst_ref=dst, send_sem=send_sem, recv_sem=recv_sem, device_id={'sp': device}, device_id_type=MESH)


def enter(devices):
    barrier = pltpu.get_barrier_semaphore()
    for device in devices:
        pl.semaphore_signal(barrier, inc=1, device_id={'sp': device}, device_id_type=MESH)
    pl.semaphore_wait(barrier, len(devices))


def project_kernel(freq_ref, len_ref, w_norm_ref, x_hbm, w_q_ref, w_k_ref, w_v_ref, q_ref, k_ref, v_ref, x_ref, x_norm, w_buf, q_buf, x_sem, w_sem, kv_sem, out_sem, send_sem, recv_sem):
    me = lax.axis_index('sp')
    core = me % 2
    partner = me + 1 - 2 * core
    num_rows, width = x_ref.shape
    head = k_ref.shape[1]
    half = q_ref.shape[1] // ROW_BLOCK // 2
    pair = 2 * head
    num_blocks = half // 2
    first_head = core * half

    def fetch(block):
        columns = pl.ds(pl.multiple_of((first_head + 2 * block) * head, pair), pair)
        return pltpu.make_async_copy(w_q_ref.at[:, columns], w_buf.at[block + 1], w_sem.at[block])

    fetch_k = pltpu.make_async_copy(w_k_ref, w_buf.at[0, :, pl.ds(0, head)], kv_sem.at[0])
    fetch_v = pltpu.make_async_copy(w_v_ref, w_buf.at[0, :, pl.ds(head, head)], kv_sem.at[1])
    fetch_x = pltpu.make_async_copy(x_hbm, x_ref, x_sem.at[0])
    fetch_x.start()
    fetch_k.start()
    fetch_v.start()
    fetch(0).start()

    gain = 1.0 + w_norm_ref[...].astype(F32)
    angles = jnp.broadcast_to(len_ref[...].astype(F32), (num_rows, num_rows)).T * freq_ref[...]
    turns = jnp.round(angles * (0.5 / np.pi))
    for part in TURN:
        angles = angles - turns * part
    cos_t = jnp.cos(angles)
    sin_t = jnp.where(lax.broadcasted_iota(jnp.int32, angles.shape, 1) < head // 2, -1.0, 1.0) * jnp.sin(angles)
    fetch_x.wait()
    for block in range(1, PROJ_WINDOW):
        fetch(block).start()

    def normalise(step, carry):
        rows = pl.ds(pl.multiple_of(step * 16, 16), 16)
        x = x_ref[rows, :].astype(F32)
        inv_rms = lax.rsqrt(jnp.mean(x * x, axis=-1, keepdims=True) + EPSILON)
        x_norm[rows, :] = (x * inv_rms * gain).astype(BF16)
        return carry

    lax.fori_loop(0, num_rows // 16, normalise, 0)

    def rotate(u):
        u = u.astype(BF16).astype(F32)
        return u * cos_t + pltpu.roll(u, head // 2, 1) * sin_t

    fetch_k.wait()
    fetch_v.wait()
    both = jnp.dot(x_norm[...], w_buf[0], preferred_element_type=F32)
    k_ref[...] = rotate(both[:, :head]).astype(BF16).astype(F32)
    v_ref[...] = both[:, head:].astype(BF16).astype(F32)
    enter([partner])

    def heads_of(c, block):
        rows = pl.multiple_of((c * half + 2 * block) * ROW_BLOCK, 2 * ROW_BLOCK)
        return q_ref.at[:, pl.ds(rows, 2 * ROW_BLOCK), :]

    def keep(block):
        return pltpu.make_async_copy(q_buf.at[block], heads_of(core, block), out_sem.at[block])

    def send(block):
        return remote(q_buf.at[block], heads_of(core, block), send_sem.at[block], recv_sem.at[block], partner)

    def step(block, carry):
        @pl.when(block + PROJ_WINDOW < num_blocks)
        def _():
            fetch(block + PROJ_WINDOW).start()

        fetch(block).wait()
        product = jnp.dot(x_norm[...], w_buf[block + 1], preferred_element_type=F32)
        for i in range(2):
            q = (rotate(product[:, i * head:(i + 1) * head]) * head ** -0.5).astype(BF16).astype(F32)
            q_buf[block, :, i * ROW_BLOCK:(i + 1) * ROW_BLOCK, :] = q.reshape(num_rows // ROW_BLOCK, ROW_BLOCK, head)
        send(block).start()
        keep(block).start()
        return carry

    lax.fori_loop(0, num_blocks, step, 0)

    def finish(block, carry):
        keep(block).wait()
        send(block).wait_send()
        other = heads_of(1 - core, block)
        remote(q_buf.at[block], other, send_sem.at[block], recv_sem.at[block], partner).wait_recv()
        return carry

    lax.fori_loop(0, num_blocks, finish, 0)


def project(hidden, w_norm, w_q, w_k, w_v, cache_len):
    num_rows, width = hidden.shape
    head = w_k.shape[1]
    heads = w_q.shape[1] // head
    inv_freq = ROPE_BASE ** (-np.arange(head // 2) * 2.0 / head)
    inv_freq = jnp.asarray(np.concatenate([inv_freq, inv_freq])[None, :], F32)
    vmem = pl.BlockSpec(memory_space=pltpu.VMEM)
    hbm = pl.BlockSpec(memory_space=pltpu.HBM)
    blocks = heads // 4
    return pl.pallas_call(
        project_kernel,
        name='project',
        out_shape=(jax.ShapeDtypeStruct((num_rows // ROW_BLOCK, heads * ROW_BLOCK, head), F32), jax.ShapeDtypeStruct((num_rows, head), F32), jax.ShapeDtypeStruct((num_rows, head), F32)),
        in_specs=[vmem, vmem, vmem, hbm, hbm, hbm, hbm],
        out_specs=(hbm, vmem, vmem),
        scratch_shapes=[
            pltpu.VMEM((num_rows, width), BF16),
            pltpu.VMEM((num_rows, width), BF16),
            pltpu.VMEM((blocks + 1, width, 2 * head), BF16),
            pltpu.VMEM((blocks, num_rows // ROW_BLOCK, 2 * ROW_BLOCK, head), F32),
            pltpu.SemaphoreType.DMA((1,)),
            pltpu.SemaphoreType.DMA((blocks,)),
            pltpu.SemaphoreType.DMA((2,)),
            pltpu.SemaphoreType.DMA((blocks,)),
            pltpu.SemaphoreType.DMA((blocks,)),
            pltpu.SemaphoreType.DMA((blocks,)),
        ],
        compiler_params=pltpu.CompilerParams(collective_id=0, has_side_effects=True, vmem_limit_bytes=60 * MIB),
    )(inv_freq, cache_len.reshape(1, -1), w_norm, hidden, w_q, w_k, w_v)


def attend_kernel(len_ref, k_new_ref, v_new_ref, q_hbm, k_hbm, v_hbm, k_out_hbm, v_out_hbm, num_hbm, stat_ref, q_ref, k_ref, v_ref, num_ref, scores_ref, factors_ref, in_sem, out_sem):
    num_rows, slots, head = k_ref.shape
    blocks = ATTEND_BLOCKS
    rows = ROW_BLOCK * blocks
    steps = num_rows // rows
    heads = stat_ref.shape[0] // 2
    base = lax.axis_index('sp') * slots
    group_iota = lax.broadcasted_iota(jnp.int32, (16, head), 0)
    lane_iota = lax.broadcasted_iota(jnp.int32, (heads, slots), 1)

    def loads(step):
        block = pl.ds(step * rows, rows)
        part = pl.ds(step * blocks, blocks)
        sem = in_sem.at[lax.rem(step, ATTEND_WINDOW + 1)]
        return [pltpu.make_async_copy(src, dst, sem) for src, dst in ((k_hbm.at[block], k_ref.at[block]), (v_hbm.at[block], v_ref.at[block]), (q_hbm.at[part], q_ref.at[part]))]

    def stores(step):
        block = pl.ds(step * rows, rows)
        part = pl.ds(step * blocks, blocks)
        return [pltpu.make_async_copy(src, dst, out_sem.at[0]) for src, dst in ((k_ref.at[block], k_out_hbm.at[block]), (v_ref.at[block], v_out_hbm.at[block]), (num_ref.at[part], num_hbm.at[part]))]

    def start(step, carry):
        for copy in loads(step):
            copy.start()
        return carry

    def attend_rows(step, carry):
        first = step * rows

        @pl.when(step + ATTEND_WINDOW < steps)
        def _():
            start(step + ATTEND_WINDOW, 0)

        for copy in loads(step):
            copy.wait()
        places = [len_ref[first + r] - base for r in range(rows)]
        for new, cache in ((k_new_ref, k_ref), (v_new_ref, v_ref)):
            fresh = new[pl.ds(pl.multiple_of(first, rows), rows), :]
            for r, p in enumerate(places):
                group = pl.multiple_of(jnp.clip(p, 0, slots - 1) // 16 * 16, 16)
                tile = cache[first + r, pl.ds(group, 16), :].astype(F32)
                cache[first + r, pl.ds(group, 16), :] = jnp.where(group_iota == p - group, fresh[r:r + 1, :], tile).astype(BF16)
        for r in range(rows):
            queries = q_ref.at[step * blocks + r // ROW_BLOCK]
            q = queries[pl.ds(r % ROW_BLOCK, heads, stride=ROW_BLOCK), :].astype(BF16)
            scores_ref[r] = lax.dot_general(q, k_ref[first + r], (((1,), (1,)), ((), ())), preferred_element_type=F32)
        stat_m = stat_ref[0:heads, :]
        stat_l = stat_ref[heads:2 * heads, :]
        for r, p in enumerate(places):
            valid = lane_iota <= p
            scores = jnp.where(valid, scores_ref[r], FLOOR)
            row_max = jnp.max(scores, axis=1, keepdims=True)
            weights = jnp.where(valid, jnp.exp(scores - row_max), 0.0)
            here = lane_iota == first + r
            stat_m = jnp.where(here, row_max, stat_m)
            stat_l = jnp.where(here, jnp.sum(weights, axis=1, keepdims=True), stat_l)
            factors_ref[r] = weights.astype(BF16)
        stat_ref[0:heads, :] = stat_m
        stat_ref[heads:2 * heads, :] = stat_l
        for r in range(rows):
            partial = num_ref.at[step * blocks + r // ROW_BLOCK]
            partial[pl.ds(r % ROW_BLOCK, heads, stride=ROW_BLOCK), :] = jnp.dot(factors_ref[r], v_ref[first + r], preferred_element_type=F32)
        for copy in stores(step):
            copy.start()
        return carry

    def finish(step, carry):
        for copy in stores(step):
            copy.wait()
        return carry

    lax.fori_loop(0, ATTEND_WINDOW, start, 0)
    lax.fori_loop(0, steps, attend_rows, 0)
    lax.fori_loop(0, steps, finish, 0)


def attend(q, k_new, v_new, k_block, v_block, cache_len):
    num_rows, slots, head = k_block.shape
    heads = q.shape[1] // ROW_BLOCK
    smem = pl.BlockSpec(memory_space=pltpu.SMEM)
    vmem = pl.BlockSpec(memory_space=pltpu.VMEM)
    hbm = pl.BlockSpec(memory_space=pltpu.HBM)
    return pl.pallas_call(
        attend_kernel,
        name='attend',
        out_shape=(jax.ShapeDtypeStruct(k_block.shape, BF16), jax.ShapeDtypeStruct(v_block.shape, BF16), jax.ShapeDtypeStruct(q.shape, F32), jax.ShapeDtypeStruct((2 * heads, num_rows), F32)),
        in_specs=[smem, vmem, vmem, hbm, hbm, hbm],
        out_specs=(hbm, hbm, hbm, vmem),
        scratch_shapes=[
            pltpu.VMEM(q.shape, F32),
            pltpu.VMEM(k_block.shape, BF16),
            pltpu.VMEM(v_block.shape, BF16),
            pltpu.VMEM(q.shape, F32),
            pltpu.VMEM((ATTEND_BLOCKS * ROW_BLOCK, heads, slots), F32),
            pltpu.VMEM((ATTEND_BLOCKS * ROW_BLOCK, heads, slots), BF16),
            pltpu.SemaphoreType.DMA((ATTEND_WINDOW + 1,)),
            pltpu.SemaphoreType.DMA((1,)),
        ],
        compiler_params=pltpu.CompilerParams(vmem_limit_bytes=60 * MIB),
    )(cache_len, k_new, v_new, q, k_block, v_block)


def combine_kernel(nz, stat_ref, num_ref, x_hbm, w_o_ref, out_hbm, x_ref, out_ref, own_num, sent_num, near_num, near_stat, part, from_long, from_short, gathered, total, attended, w_buf, x_sem, out_sem, own_sem, w_sem, stat_sem, near_send, near_recv, long_send, long_recv, short_send, short_recv, far_send, far_recv, back_send, back_recv, side_send, side_recv):
    me = lax.axis_index('sp')
    z = me // 2
    core = me % 2
    partner = me + 1 - 2 * core
    way = 1 - 2 * core
    num_rows, width = x_ref.shape
    heads = num_ref.shape[1] // ROW_BLOCK
    head = num_ref.shape[2]
    share = heads // (2 * nz)
    far = nz // 2

    def device(chip, c):
        return (chip + 2 * nz) % nz * 2 + c

    ahead = device(z + way, core)
    behind = device(z - way, core)
    targets = [far]
    for hop in range(far - 1, 0, -1):
        targets += [-hop, hop]
    targets.append(0)
    sources = [0]
    for hop in range(1, far):
        sources += [-hop, hop]
    sources.append(-far)

    units = [(0, s) for s in range(share)]
    for hop in range(1, far):
        units += [(sources.index(step), s) for s in range(share) for step in (-hop, hop)]
    units += [(nz - 1, s) for s in range(share)]

    def fetch(u):
        k, s = units[u]
        chip = z + way * sources[k]
        rows = [pl.ds(pl.multiple_of((device(chip, c) * share + s) * head, head), head) for c in range(2)]
        return [pltpu.make_async_copy(w_o_ref.at[rows[c], :], w_buf.at[u % OUT_SLOTS, c * head:(c + 1) * head, :], w_sem.at[u % OUT_SLOTS, c]) for c in range(2)]

    def start_fetch(u):
        for copy in fetch(u):
            copy.start()

    def own_heads(i, c):
        way_c = way * (1 - 2 * c)
        rows = share * ROW_BLOCK
        first = rows * device(z + way_c * targets[i], core + way * c)
        return num_ref.at[:, pl.ds(pl.multiple_of(first, rows), rows), :]

    def stage(i):
        return [pltpu.make_async_copy(own_heads(i, 1), sent_num.at[i], own_sem.at[1, i]), pltpu.make_async_copy(own_heads(i, 0), own_num.at[i], own_sem.at[0, i])]

    stages = [stage(i) for i in range(nz)]
    swap_stat = remote(stat_ref, near_stat, stat_sem.at[0], stat_sem.at[1], partner)
    swaps = [remote(sent_num.at[i], near_num.at[i], near_send.at[i], near_recv.at[i], partner) for i in range(nz)]

    def start_swaps(low, high):
        for i in range(low, high):
            stages[i][0].wait()
            swaps[i].start()

    for i in range(2):
        for copy in stages[i]:
            copy.start()
    enter([partner, ahead, behind])
    swap_stat.start()
    start_swaps(0, 2)
    for i in range(2, nz):
        for copy in stages[i]:
            copy.start()
    start_swaps(2, 4)
    fetch_x = pltpu.make_async_copy(x_hbm, x_ref, x_sem.at[0])
    ahead_of_use = list(range(OUT_SLOTS))

    def fetch_some(count):
        for _ in range(count):
            if ahead_of_use:
                start_fetch(ahead_of_use.pop(0))

    def column(row):
        return jnp.broadcast_to(row, (num_rows, num_rows)).T

    def merge(a, b):
        (x_a, m_a, l_a), (x_b, m_b, l_b) = a, b
        m = jnp.maximum(m_a, m_b)
        scale_a = jnp.exp(m_a - m)
        scale_b = jnp.exp(m_b - m)
        return x_a * column(scale_a) + x_b * column(scale_b), m, l_a * scale_a + l_b * scale_b

    def load(ref):
        return ref[0:num_rows, :], ref[num_rows:num_rows + 1, :], ref[num_rows + 1:num_rows + 2, :]

    sub_iota = lax.broadcasted_iota(jnp.int32, (8, num_rows), 0)

    def store(ref, triple):
        x, m, l = triple
        ref[0:num_rows, :] = x
        ref[num_rows:num_rows + 8, :] = jnp.where(sub_iota == 0, m, l)

    def own(i, send=None):
        stages[i][1].wait()
        swaps[i].wait_recv()
        first = share * device(z + way * targets[i], core)
        for s in range(share):
            h = first + s
            rows = slice(s * ROW_BLOCK, (s + 1) * ROW_BLOCK)
            mine = (own_num[i, :, rows, :].reshape(num_rows, head), stat_ref[pl.ds(h, 1), :], stat_ref[pl.ds(heads + h, 1), :])
            theirs = (near_num[i, :, rows, :].reshape(num_rows, head), near_stat[pl.ds(h, 1), :], near_stat[pl.ds(heads + h, 1), :])
            store(part.at[i, s], merge(mine, theirs))
            if send is not None:
                send(0, s).start()

    def long_copy(hop, s):
        i = 0 if hop == 0 else 2 * hop
        return remote(part.at[i, s], from_long.at[hop, s], long_send.at[hop, s], long_recv.at[hop, s], ahead)

    def short_copy(hop, s):
        return remote(part.at[2 * hop + 1, s], from_short.at[hop, s], short_send.at[hop, s], short_recv.at[hop, s], behind)

    swap_stat.wait_recv()
    for hop in range(far):
        if hop == 0:
            own(0, long_copy)
            own(1, short_copy)
            start_swaps(4, nz)
            fetch_x.start()
            fetch_some(2)
            continue
        own(2 * hop)
        own(2 * hop + 1)
        for s in range(share):
            long_copy(hop - 1, s).wait_recv()
            store(part.at[2 * hop, s], merge(load(part.at[2 * hop, s]), load(from_long.at[hop - 1, s])))
            long_copy(hop, s).start()
            fetch_some(2)
            if hop < far - 1:
                short_copy(hop - 1, s).wait_recv()
                store(part.at[2 * hop + 1, s], merge(load(part.at[2 * hop + 1, s]), load(from_short.at[hop - 1, s])))
                short_copy(hop, s).start()

    def far_copy(hop, s):
        slot = gathered.at[device(z - way * hop, core), s]
        return remote(slot, slot, far_send.at[hop, s], far_recv.at[hop, s], ahead)

    def back_copy(hop, s):
        slot = gathered.at[device(z + way * hop, core), s]
        return remote(slot, slot, back_send.at[hop, s], back_recv.at[hop, s], behind)

    def side_copy(k, s):
        slot = gathered.at[device(z + way * sources[k], core), s]
        return remote(slot, slot, side_send.at[k, s], side_recv.at[k, s], partner)

    def far_arrival(hop, s):
        slot = gathered.at[device(z - way * (hop + 1), core), s]
        return remote(slot, slot, far_send.at[hop, s], far_recv.at[hop, s], ahead)

    def back_arrival(hop, s):
        slot = gathered.at[device(z + way * (hop + 1), core), s]
        return remote(slot, slot, back_send.at[hop, s], back_recv.at[hop, s], behind)

    def side_arrival(k, s):
        slot = gathered.at[device(z - way * sources[k], 1 - core), s]
        return remote(slot, slot, side_send.at[k, s], side_recv.at[k, s], partner)

    mirror = {hop: k for k, hop in enumerate(sources)}
    mirror[far] = mirror[-far]

    last = far - 1
    fetch_some(OUT_SLOTS)
    for s in range(share):
        short_copy(last - 1, s).wait_recv()
        triple = merge(load(part.at[2 * far - 1, s]), load(from_short.at[last - 1, s]))
        long_copy(last, s).wait_recv()
        x, _, l = merge(triple, load(from_long.at[last, s]))
        gathered[me, s] = (x / column(l)).astype(BF16).astype(F32)
        far_copy(0, s).start()
        back_copy(0, s).start()
        side_copy(0, s).start()

    tiles = width // OUT_TILE

    def save(n):
        columns = pl.ds(pl.multiple_of(n * OUT_TILE, OUT_TILE), OUT_TILE)
        return pltpu.make_async_copy(out_ref.at[:, columns], out_hbm.at[:, columns], out_sem.at[n])

    def multiply(us):
        for i, u in enumerate(us):
            k, s = units[u]
            side_arrival(mirror[-sources[k]], s).wait_recv()
            chip = z + way * sources[k]
            for c in range(2):
                attended[i, :, c * head:(c + 1) * head] = gathered[device(chip, c), s].astype(BF16)
            for copy in fetch(u):
                copy.wait()

        def tile(n, carry):
            columns = pl.ds(pl.multiple_of(n * OUT_TILE, OUT_TILE), OUT_TILE)
            product = None
            for i, u in enumerate(us):
                term = jnp.dot(attended[i], w_buf[u % OUT_SLOTS, :, columns], preferred_element_type=F32)
                product = term if product is None else product + term
            before = x_ref[:, columns].astype(F32) if 0 in us else total[:, columns]
            if len(units) - 1 in us:
                out_ref[:, columns] = (before + product).astype(BF16)
                save(n).start()
            else:
                total[:, columns] = before + product
            return carry

        lax.fori_loop(0, tiles, tile, 0)
        for u in us:
            if u + OUT_SLOTS < len(units):
                start_fetch(u + OUT_SLOTS)

    chunks = [[s] for s in range(share)]
    while sum(map(len, chunks)) < len(units) - share:
        u = sum(map(len, chunks))
        chunks.append([u, u + 1])
    chunks += [[len(units) - share + s] for s in range(share)]
    fetch_x.wait()
    multiply(chunks.pop(0))
    multiply(chunks.pop(0))
    for hop in range(far):
        for s in range(share):
            far_arrival(hop, s).wait_recv()
            if hop < far - 1:
                far_copy(hop + 1, s).start()
            side_copy(mirror[-(hop + 1)], s).start()
            if hop < far - 1:
                back_arrival(hop, s).wait_recv()
                if hop < far - 2:
                    back_copy(hop + 1, s).start()
                side_copy(mirror[hop + 1], s).start()
            multiply(chunks.pop(0))
    for chunk in chunks:
        multiply(chunk)
    for n in range(tiles):
        save(n).wait()

    swap_stat.wait_send()
    for swap in swaps:
        swap.wait_send()
    for s in range(share):
        for hop in range(far):
            long_copy(hop, s).wait_send()
            far_copy(hop, s).wait_send()
            if hop < far - 1:
                short_copy(hop, s).wait_send()
                back_copy(hop, s).wait_send()
        for k in range(nz):
            side_copy(k, s).wait_send()


def combine(num, stat, hidden, w_o, group):
    num_rows, width = hidden.shape
    heads = num.shape[1] // ROW_BLOCK
    head = num.shape[2]
    nz = group // 2
    share = heads // group
    far = nz // 2
    vmem = pl.BlockSpec(memory_space=pltpu.VMEM)
    hbm = pl.BlockSpec(memory_space=pltpu.HBM)
    dma = pltpu.SemaphoreType.DMA
    piece = (num_rows + 8, head)
    return pl.pallas_call(
        functools.partial(combine_kernel, nz),
        name='combine',
        out_shape=jax.ShapeDtypeStruct((num_rows, width), BF16),
        in_specs=[vmem, hbm, hbm, hbm],
        out_specs=hbm,
        scratch_shapes=[
            pltpu.VMEM((num_rows, width), BF16),
            pltpu.VMEM((num_rows, width), BF16),
            pltpu.VMEM((nz, num_rows // ROW_BLOCK, share * ROW_BLOCK, head), F32),
            pltpu.VMEM((nz, num_rows // ROW_BLOCK, share * ROW_BLOCK, head), F32),
            pltpu.VMEM((nz, num_rows // ROW_BLOCK, share * ROW_BLOCK, head), F32),
            pltpu.VMEM((2 * heads, num_rows), F32),
            pltpu.VMEM((nz, share) + piece, F32),
            pltpu.VMEM((far, share) + piece, F32),
            pltpu.VMEM((far - 1, share) + piece, F32),
            pltpu.VMEM((group, share, num_rows, head), F32),
            pltpu.VMEM((num_rows, width), F32),
            pltpu.VMEM((2, num_rows, 2 * head), BF16),
            pltpu.VMEM((OUT_SLOTS, 2 * head, width), BF16),
            dma((1,)),
            dma((width // OUT_TILE,)),
            dma((2, nz)),
            dma((OUT_SLOTS, 2)),
            dma((2,)),
            dma((nz,)),
            dma((nz,)),
            dma((far, share)),
            dma((far, share)),
            dma((far - 1, share)),
            dma((far - 1, share)),
            dma((far, share)),
            dma((far, share)),
            dma((far - 1, share)),
            dma((far - 1, share)),
            dma((nz, share)),
            dma((nz, share)),
        ],
        compiler_params=pltpu.CompilerParams(collective_id=1, has_side_effects=True, vmem_limit_bytes=62 * MIB),
    )(stat, num, hidden, w_o)


def solution(mesh):
    group = mesh.shape['sp']

    def local_step(hidden, w_norm, w_q, w_k, w_v, w_o, k_block, v_block, cache_len):
        q, k_new, v_new = project(hidden, w_norm, w_q, w_k, w_v, cache_len)
        k_out, v_out, num, stat = attend(q, k_new, v_new, k_block, v_block, cache_len)
        out = combine(num, stat, hidden, w_o, group)
        return out, k_out, v_out

    cache_spec = P('dp', 'sp', None)
    return jax.shard_map(local_step, mesh=mesh, in_specs=(P('dp', None), P(None), P(None, None), P(None, None), P(None, None), P(None, None), cache_spec, cache_spec, P('dp')), out_specs=(P('dp', None), cache_spec, cache_spec), check_vma=False)
```

```python
import functools

import jax
import jax.numpy as jnp
import numpy as np
from jax import lax
from jax.experimental import pallas as pl
from jax.experimental.pallas import tpu as pltpu
from jax.sharding import PartitionSpec as P

ROPE_BASE = 10000.0
EPSILON = 1e-6
MIB = 1024 * 1024
F32 = jnp.float32
BF16 = jnp.bfloat16
FLOOR = float(np.finfo(np.float32).min)
MESH = pl.DeviceIdType.MESH
TURN = (6.28125, 0.0019340515136718750, float(2 * np.pi - 6.28125 - 0.0019340515136718750))
ROW_BLOCK = 8
OUT_SLOTS = 12
PROJ_WINDOW = 4
ATTEND_WINDOW = 3
ATTEND_BLOCKS = 2
OUT_TILE = 3072


def remote(src, dst, send_sem, recv_sem, device):
    return pltpu.make_async_remote_copy(src_ref=src, dst_ref=dst, send_sem=send_sem, recv_sem=recv_sem, device_id={'sp': device}, device_id_type=MESH)


def enter(devices):
    barrier = pltpu.get_barrier_semaphore()
    for device in devices:
        pl.semaphore_signal(barrier, inc=1, device_id={'sp': device}, device_id_type=MESH)
    pl.semaphore_wait(barrier, len(devices))


def project_kernel(freq_ref, len_ref, w_norm_ref, x_hbm, w_q_ref, w_k_ref, w_v_ref, q_ref, k_ref, v_ref, x_ref, x_norm, w_buf, q_buf, x_sem, w_sem, kv_sem, out_sem, send_sem, recv_sem):
    me = lax.axis_index('sp')
    core = me % 2
    partner = me + 1 - 2 * core
    num_rows, width = x_ref.shape
    head = k_ref.shape[1]
    half = q_ref.shape[1] // ROW_BLOCK // 2
    pair = 2 * head
    num_blocks = half // 2
    first_head = core * half

    def fetch(block):
        columns = pl.ds(pl.multiple_of((first_head + 2 * block) * head, pair), pair)
        return pltpu.make_async_copy(w_q_ref.at[:, columns], w_buf.at[block + 1], w_sem.at[block])

    fetch_k = pltpu.make_async_copy(w_k_ref, w_buf.at[0, :, pl.ds(0, head)], kv_sem.at[0])
    fetch_v = pltpu.make_async_copy(w_v_ref, w_buf.at[0, :, pl.ds(head, head)], kv_sem.at[1])
    fetch_x = pltpu.make_async_copy(x_hbm, x_ref, x_sem.at[0])
    fetch_x.start()
    fetch(0).start()
    fetch(1).start()

    gain = 1.0 + w_norm_ref[...].astype(F32)
    angles = jnp.broadcast_to(len_ref[...].astype(F32), (num_rows, num_rows)).T * freq_ref[...]
    turns = jnp.round(angles * (0.5 / np.pi))
    for part in TURN:
        angles = angles - turns * part
    cos_t = jnp.cos(angles)
    sin_t = jnp.where(lax.broadcasted_iota(jnp.int32, angles.shape, 1) < head // 2, -1.0, 1.0) * jnp.sin(angles)
    fetch_x.wait()
    for block in range(2, PROJ_WINDOW):
        fetch(block).start()

    def normalise(step, carry):
        rows = pl.ds(pl.multiple_of(step * 16, 16), 16)
        x = x_ref[rows, :].astype(F32)
        inv_rms = lax.rsqrt(jnp.mean(x * x, axis=-1, keepdims=True) + EPSILON)
        x_norm[rows, :] = (x * inv_rms * gain).astype(BF16)
        return carry

    lax.fori_loop(0, num_rows // 16, normalise, 0)

    def rotate(u):
        u = u.astype(BF16).astype(F32)
        return u * cos_t + pltpu.roll(u, head // 2, 1) * sin_t

    enter([partner])

    def heads_of(c, block):
        rows = pl.multiple_of((c * half + 2 * block) * ROW_BLOCK, 2 * ROW_BLOCK)
        return q_ref.at[:, pl.ds(rows, 2 * ROW_BLOCK), :]

    def keep(block):
        return pltpu.make_async_copy(q_buf.at[block], heads_of(core, block), out_sem.at[block])

    def send(block):
        return remote(q_buf.at[block], heads_of(core, block), send_sem.at[block], recv_sem.at[block], partner)

    def step(block, carry):
        @pl.when(block + PROJ_WINDOW < num_blocks)
        def _():
            fetch(block + PROJ_WINDOW).start()

        @pl.when(block + PROJ_WINDOW == num_blocks)
        def _():
            fetch_k.start()
            fetch_v.start()

        fetch(block).wait()
        product = jnp.dot(x_norm[...], w_buf[block + 1], preferred_element_type=F32)
        for i in range(2):
            q = (rotate(product[:, i * head:(i + 1) * head]) * head ** -0.5).astype(BF16).astype(F32)
            q_buf[block, :, i * ROW_BLOCK:(i + 1) * ROW_BLOCK, :] = q.reshape(num_rows // ROW_BLOCK, ROW_BLOCK, head)
        send(block).start()
        keep(block).start()
        return carry

    lax.fori_loop(0, num_blocks, step, 0)
    fetch_k.wait()
    fetch_v.wait()
    both = jnp.dot(x_norm[...], w_buf[0], preferred_element_type=F32)
    k_ref[...] = rotate(both[:, :head]).astype(BF16).astype(F32)
    v_ref[...] = both[:, head:].astype(BF16).astype(F32)

    def finish(block, carry):
        keep(block).wait()
        send(block).wait_send()
        other = heads_of(1 - core, block)
        remote(q_buf.at[block], other, send_sem.at[block], recv_sem.at[block], partner).wait_recv()
        return carry

    lax.fori_loop(0, num_blocks, finish, 0)


def project(hidden, w_norm, w_q, w_k, w_v, cache_len):
    num_rows, width = hidden.shape
    head = w_k.shape[1]
    heads = w_q.shape[1] // head
    inv_freq = ROPE_BASE ** (-np.arange(head // 2) * 2.0 / head)
    inv_freq = jnp.asarray(np.concatenate([inv_freq, inv_freq])[None, :], F32)
    vmem = pl.BlockSpec(memory_space=pltpu.VMEM)
    hbm = pl.BlockSpec(memory_space=pltpu.HBM)
    blocks = heads // 4
    return pl.pallas_call(
        project_kernel,
        name='project',
        out_shape=(jax.ShapeDtypeStruct((num_rows // ROW_BLOCK, heads * ROW_BLOCK, head), F32), jax.ShapeDtypeStruct((num_rows, head), F32), jax.ShapeDtypeStruct((num_rows, head), F32)),
        in_specs=[vmem, vmem, vmem, hbm, hbm, hbm, hbm],
        out_specs=(hbm, vmem, vmem),
        scratch_shapes=[
            pltpu.VMEM((num_rows, width), BF16),
            pltpu.VMEM((num_rows, width), BF16),
            pltpu.VMEM((blocks + 1, width, 2 * head), BF16),
            pltpu.VMEM((blocks, num_rows // ROW_BLOCK, 2 * ROW_BLOCK, head), F32),
            pltpu.SemaphoreType.DMA((1,)),
            pltpu.SemaphoreType.DMA((blocks,)),
            pltpu.SemaphoreType.DMA((2,)),
            pltpu.SemaphoreType.DMA((blocks,)),
            pltpu.SemaphoreType.DMA((blocks,)),
            pltpu.SemaphoreType.DMA((blocks,)),
        ],
        compiler_params=pltpu.CompilerParams(collective_id=0, has_side_effects=True, vmem_limit_bytes=60 * MIB),
    )(inv_freq, cache_len.reshape(1, -1), w_norm, hidden, w_q, w_k, w_v)


def attend_kernel(len_ref, k_new_ref, v_new_ref, q_hbm, k_hbm, v_hbm, k_out_hbm, v_out_hbm, num_hbm, stat_ref, q_ref, k_ref, v_ref, num_ref, scores_ref, factors_ref, in_sem, out_sem):
    num_rows, slots, head = k_ref.shape
    blocks = ATTEND_BLOCKS
    rows = ROW_BLOCK * blocks
    steps = num_rows // rows
    heads = stat_ref.shape[0] // 2
    base = lax.axis_index('sp') * slots
    group_iota = lax.broadcasted_iota(jnp.int32, (16, head), 0)
    lane_iota = lax.broadcasted_iota(jnp.int32, (heads, slots), 1)

    def loads(step):
        block = pl.ds(step * rows, rows)
        part = pl.ds(step * blocks, blocks)
        sem = in_sem.at[lax.rem(step, ATTEND_WINDOW + 1)]
        return [pltpu.make_async_copy(src, dst, sem) for src, dst in ((k_hbm.at[block], k_ref.at[block]), (v_hbm.at[block], v_ref.at[block]), (q_hbm.at[part], q_ref.at[part]))]

    def store_caches(step):
        block = pl.ds(step * rows, rows)
        return [pltpu.make_async_copy(src, dst, out_sem.at[0]) for src, dst in ((k_ref.at[block], k_out_hbm.at[block]), (v_ref.at[block], v_out_hbm.at[block]))]

    def store_partial(step):
        part = pl.ds(step * blocks, blocks)
        return pltpu.make_async_copy(num_ref.at[part], num_hbm.at[part], out_sem.at[0])

    def start(step, carry):
        for copy in loads(step):
            copy.start()
        return carry

    def attend_rows(step, carry):
        first = step * rows

        for copy in loads(step):
            copy.wait()

        @pl.when(step == 0)
        def _():
            start(ATTEND_WINDOW - 1, 0)

        @pl.when(step + ATTEND_WINDOW < steps)
        def _():
            start(step + ATTEND_WINDOW, 0)

        places = [len_ref[first + r] - base for r in range(rows)]
        for new, cache in ((k_new_ref, k_ref), (v_new_ref, v_ref)):
            fresh = new[pl.ds(pl.multiple_of(first, rows), rows), :]
            for r, p in enumerate(places):
                group = pl.multiple_of(jnp.clip(p, 0, slots - 1) // 16 * 16, 16)
                tile = cache[first + r, pl.ds(group, 16), :].astype(F32)
                cache[first + r, pl.ds(group, 16), :] = jnp.where(group_iota == p - group, fresh[r:r + 1, :], tile).astype(BF16)
        for r in range(rows):
            queries = q_ref.at[step * blocks + r // ROW_BLOCK]
            q = queries[pl.ds(r % ROW_BLOCK, heads, stride=ROW_BLOCK), :].astype(BF16)
            scores_ref[r] = lax.dot_general(q, k_ref[first + r], (((1,), (1,)), ((), ())), preferred_element_type=F32)
        for copy in store_caches(step):
            copy.start()
        stat_m = stat_ref[0:heads, :]
        stat_l = stat_ref[heads:2 * heads, :]
        for r, p in enumerate(places):
            valid = lane_iota <= p
            scores = jnp.where(valid, scores_ref[r], FLOOR)
            row_max = jnp.max(scores, axis=1, keepdims=True)
            weights = jnp.where(valid, jnp.exp(scores - row_max), 0.0)
            here = lane_iota == first + r
            stat_m = jnp.where(here, row_max, stat_m)
            stat_l = jnp.where(here, jnp.sum(weights, axis=1, keepdims=True), stat_l)
            factors_ref[r] = weights.astype(BF16)
        stat_ref[0:heads, :] = stat_m
        stat_ref[heads:2 * heads, :] = stat_l
        for r in range(rows):
            partial = num_ref.at[step * blocks + r // ROW_BLOCK]
            partial[pl.ds(r % ROW_BLOCK, heads, stride=ROW_BLOCK), :] = jnp.dot(factors_ref[r], v_ref[first + r], preferred_element_type=F32)
        store_partial(step).start()
        return carry

    def finish(step, carry):
        for copy in store_caches(step):
            copy.wait()
        store_partial(step).wait()
        return carry

    lax.fori_loop(0, ATTEND_WINDOW - 1, start, 0)
    lax.fori_loop(0, steps, attend_rows, 0)
    lax.fori_loop(0, steps, finish, 0)


def attend(q, k_new, v_new, k_block, v_block, cache_len):
    num_rows, slots, head = k_block.shape
    heads = q.shape[1] // ROW_BLOCK
    smem = pl.BlockSpec(memory_space=pltpu.SMEM)
    vmem = pl.BlockSpec(memory_space=pltpu.VMEM)
    hbm = pl.BlockSpec(memory_space=pltpu.HBM)
    return pl.pallas_call(
        attend_kernel,
        name='attend',
        out_shape=(jax.ShapeDtypeStruct(k_block.shape, BF16), jax.ShapeDtypeStruct(v_block.shape, BF16), jax.ShapeDtypeStruct(q.shape, F32), jax.ShapeDtypeStruct((2 * heads, num_rows), F32)),
        in_specs=[smem, vmem, vmem, hbm, hbm, hbm],
        out_specs=(hbm, hbm, hbm, vmem),
        scratch_shapes=[
            pltpu.VMEM(q.shape, F32),
            pltpu.VMEM(k_block.shape, BF16),
            pltpu.VMEM(v_block.shape, BF16),
            pltpu.VMEM(q.shape, F32),
            pltpu.VMEM((ATTEND_BLOCKS * ROW_BLOCK, heads, slots), F32),
            pltpu.VMEM((ATTEND_BLOCKS * ROW_BLOCK, heads, slots), BF16),
            pltpu.SemaphoreType.DMA((ATTEND_WINDOW + 1,)),
            pltpu.SemaphoreType.DMA((1,)),
        ],
        compiler_params=pltpu.CompilerParams(vmem_limit_bytes=60 * MIB),
    )(cache_len, k_new, v_new, q, k_block, v_block)


def combine_kernel(nz, stat_ref, num_ref, x_hbm, w_o_ref, out_hbm, x_ref, out_ref, own_num, sent_num, near_num, near_stat, part, from_long, from_short, gathered, total, attended, w_buf, x_sem, out_sem, own_sem, w_sem, stat_sem, near_send, near_recv, long_send, long_recv, short_send, short_recv, far_send, far_recv, back_send, back_recv, side_send, side_recv):
    me = lax.axis_index('sp')
    z = me // 2
    core = me % 2
    partner = me + 1 - 2 * core
    way = 1 - 2 * core
    num_rows, width = x_ref.shape
    heads = num_ref.shape[1] // ROW_BLOCK
    head = num_ref.shape[2]
    share = heads // (2 * nz)
    far = nz // 2

    def device(chip, c):
        return (chip + 2 * nz) % nz * 2 + c

    ahead = device(z + way, core)
    behind = device(z - way, core)
    targets = [far]
    for hop in range(far - 1, 0, -1):
        targets += [-hop, hop]
    targets.append(0)
    sources = [0]
    for hop in range(1, far):
        sources += [-hop, hop]
    sources.append(-far)

    units = [(0, s) for s in range(share)]
    for hop in range(1, far):
        units += [(sources.index(step), s) for s in range(share) for step in (-hop, hop)]
    units += [(nz - 1, s) for s in range(share)]

    def fetch(u):
        k, s = units[u]
        chip = z + way * sources[k]
        rows = [pl.ds(pl.multiple_of((device(chip, c) * share + s) * head, head), head) for c in range(2)]
        return [pltpu.make_async_copy(w_o_ref.at[rows[c], :], w_buf.at[u % OUT_SLOTS, c * head:(c + 1) * head, :], w_sem.at[u % OUT_SLOTS, c]) for c in range(2)]

    def start_fetch(u):
        for copy in fetch(u):
            copy.start()

    def own_heads(i, c):
        way_c = way * (1 - 2 * c)
        rows = share * ROW_BLOCK
        first = rows * device(z + way_c * targets[i], core + way * c)
        return num_ref.at[:, pl.ds(pl.multiple_of(first, rows), rows), :]

    def stage(i):
        return [pltpu.make_async_copy(own_heads(i, 1), sent_num.at[i], own_sem.at[1, i]), pltpu.make_async_copy(own_heads(i, 0), own_num.at[i], own_sem.at[0, i])]

    stages = [stage(i) for i in range(nz)]
    swap_stat = remote(stat_ref, near_stat, stat_sem.at[0], stat_sem.at[1], partner)
    swaps = [remote(sent_num.at[i], near_num.at[i], near_send.at[i], near_recv.at[i], partner) for i in range(nz)]

    def start_swaps(low, high):
        for i in range(low, high):
            stages[i][0].wait()
            swaps[i].start()

    for i in range(2):
        for copy in stages[i]:
            copy.start()
    enter([partner, ahead, behind])
    swap_stat.start()
    start_swaps(0, 2)
    for i in range(2, nz):
        for copy in stages[i]:
            copy.start()
    start_swaps(2, 4)
    fetch_x = pltpu.make_async_copy(x_hbm, x_ref, x_sem.at[0])
    ahead_of_use = list(range(OUT_SLOTS))

    def fetch_some(count):
        for _ in range(count):
            if ahead_of_use:
                start_fetch(ahead_of_use.pop(0))

    def column(row):
        return jnp.broadcast_to(row, (num_rows, num_rows)).T

    def merge(a, b):
        (x_a, m_a, l_a), (x_b, m_b, l_b) = a, b
        m = jnp.maximum(m_a, m_b)
        scale_a = jnp.exp(m_a - m)
        scale_b = jnp.exp(m_b - m)
        return x_a * column(scale_a) + x_b * column(scale_b), m, l_a * scale_a + l_b * scale_b

    def load(ref):
        return ref[0:num_rows, :], ref[num_rows:num_rows + 1, :], ref[num_rows + 1:num_rows + 2, :]

    sub_iota = lax.broadcasted_iota(jnp.int32, (8, num_rows), 0)

    def store(ref, triple):
        x, m, l = triple
        ref[0:num_rows, :] = x
        ref[num_rows:num_rows + 8, :] = jnp.where(sub_iota == 0, m, l)

    def own(i, send=None):
        stages[i][1].wait()
        swaps[i].wait_recv()
        first = share * device(z + way * targets[i], core)
        for s in range(share):
            h = first + s
            rows = slice(s * ROW_BLOCK, (s + 1) * ROW_BLOCK)
            mine = (own_num[i, :, rows, :].reshape(num_rows, head), stat_ref[pl.ds(h, 1), :], stat_ref[pl.ds(heads + h, 1), :])
            theirs = (near_num[i, :, rows, :].reshape(num_rows, head), near_stat[pl.ds(h, 1), :], near_stat[pl.ds(heads + h, 1), :])
            store(part.at[i, s], merge(mine, theirs))
            if send is not None:
                send(0, s).start()

    def long_copy(hop, s):
        i = 0 if hop == 0 else 2 * hop
        return remote(part.at[i, s], from_long.at[hop, s], long_send.at[hop, s], long_recv.at[hop, s], ahead)

    def short_copy(hop, s):
        return remote(part.at[2 * hop + 1, s], from_short.at[hop, s], short_send.at[hop, s], short_recv.at[hop, s], behind)

    swap_stat.wait_recv()
    for hop in range(far):
        if hop == 0:
            own(0, long_copy)
            own(1, short_copy)
            start_swaps(4, nz)
            fetch_x.start()
            fetch_some(2)
            continue
        own(2 * hop)
        own(2 * hop + 1)
        for s in range(share):
            long_copy(hop - 1, s).wait_recv()
            store(part.at[2 * hop, s], merge(load(part.at[2 * hop, s]), load(from_long.at[hop - 1, s])))
            long_copy(hop, s).start()
            fetch_some(2)
            if hop < far - 1:
                short_copy(hop - 1, s).wait_recv()
                store(part.at[2 * hop + 1, s], merge(load(part.at[2 * hop + 1, s]), load(from_short.at[hop - 1, s])))
                short_copy(hop, s).start()

    def far_copy(hop, s):
        slot = gathered.at[device(z - way * hop, core), s]
        return remote(slot, slot, far_send.at[hop, s], far_recv.at[hop, s], ahead)

    def back_copy(hop, s):
        slot = gathered.at[device(z + way * hop, core), s]
        return remote(slot, slot, back_send.at[hop, s], back_recv.at[hop, s], behind)

    def side_copy(k, s):
        slot = gathered.at[device(z + way * sources[k], core), s]
        return remote(slot, slot, side_send.at[k, s], side_recv.at[k, s], partner)

    def far_arrival(hop, s):
        slot = gathered.at[device(z - way * (hop + 1), core), s]
        return remote(slot, slot, far_send.at[hop, s], far_recv.at[hop, s], ahead)

    def back_arrival(hop, s):
        slot = gathered.at[device(z + way * (hop + 1), core), s]
        return remote(slot, slot, back_send.at[hop, s], back_recv.at[hop, s], behind)

    def side_arrival(k, s):
        slot = gathered.at[device(z - way * sources[k], 1 - core), s]
        return remote(slot, slot, side_send.at[k, s], side_recv.at[k, s], partner)

    mirror = {hop: k for k, hop in enumerate(sources)}
    mirror[far] = mirror[-far]

    last = far - 1
    fetch_some(OUT_SLOTS)
    for s in range(share):
        short_copy(last - 1, s).wait_recv()
        triple = merge(load(part.at[2 * far - 1, s]), load(from_short.at[last - 1, s]))
        long_copy(last, s).wait_recv()
        x, _, l = merge(triple, load(from_long.at[last, s]))
        gathered[me, s] = (x / column(l)).astype(BF16).astype(F32)
        far_copy(0, s).start()
        back_copy(0, s).start()
        side_copy(0, s).start()

    tiles = width // OUT_TILE

    def save(n):
        columns = pl.ds(pl.multiple_of(n * OUT_TILE, OUT_TILE), OUT_TILE)
        return pltpu.make_async_copy(out_ref.at[:, columns], out_hbm.at[:, columns], out_sem.at[n])

    def multiply(us):
        for i, u in enumerate(us):
            k, s = units[u]
            side_arrival(mirror[-sources[k]], s).wait_recv()
            chip = z + way * sources[k]
            for c in range(2):
                attended[i, :, c * head:(c + 1) * head] = gathered[device(chip, c), s].astype(BF16)
            for copy in fetch(u):
                copy.wait()

        def tile(n, carry):
            columns = pl.ds(pl.multiple_of(n * OUT_TILE, OUT_TILE), OUT_TILE)
            product = None
            for i, u in enumerate(us):
                term = jnp.dot(attended[i], w_buf[u % OUT_SLOTS, :, columns], preferred_element_type=F32)
                product = term if product is None else product + term
            before = x_ref[:, columns].astype(F32) if 0 in us else total[:, columns]
            if len(units) - 1 in us:
                out_ref[:, columns] = (before + product).astype(BF16)
                save(n).start()
            else:
                total[:, columns] = before + product
            return carry

        lax.fori_loop(0, tiles, tile, 0)
        for u in us:
            if u + OUT_SLOTS < len(units):
                start_fetch(u + OUT_SLOTS)

    chunks = [[s] for s in range(share)]
    while sum(map(len, chunks)) < len(units) - share:
        u = sum(map(len, chunks))
        chunks.append([u, u + 1])
    chunks += [[len(units) - share + s] for s in range(share)]
    fetch_x.wait()
    multiply(chunks.pop(0))
    multiply(chunks.pop(0))
    for hop in range(far):
        for s in range(share):
            far_arrival(hop, s).wait_recv()
            if hop < far - 1:
                far_copy(hop + 1, s).start()
            side_copy(mirror[-(hop + 1)], s).start()
            if hop < far - 1:
                back_arrival(hop, s).wait_recv()
                if hop < far - 2:
                    back_copy(hop + 1, s).start()
                side_copy(mirror[hop + 1], s).start()
            multiply(chunks.pop(0))
    for chunk in chunks:
        multiply(chunk)
    for n in range(tiles):
        save(n).wait()

    swap_stat.wait_send()
    for swap in swaps:
        swap.wait_send()
    for s in range(share):
        for hop in range(far):
            long_copy(hop, s).wait_send()
            far_copy(hop, s).wait_send()
            if hop < far - 1:
                short_copy(hop, s).wait_send()
                back_copy(hop, s).wait_send()
        for k in range(nz):
            side_copy(k, s).wait_send()


def combine(num, stat, hidden, w_o, group):
    num_rows, width = hidden.shape
    heads = num.shape[1] // ROW_BLOCK
    head = num.shape[2]
    nz = group // 2
    share = heads // group
    far = nz // 2
    vmem = pl.BlockSpec(memory_space=pltpu.VMEM)
    hbm = pl.BlockSpec(memory_space=pltpu.HBM)
    dma = pltpu.SemaphoreType.DMA
    piece = (num_rows + 8, head)
    return pl.pallas_call(
        functools.partial(combine_kernel, nz),
        name='combine',
        out_shape=jax.ShapeDtypeStruct((num_rows, width), BF16),
        in_specs=[vmem, hbm, hbm, hbm],
        out_specs=hbm,
        scratch_shapes=[
            pltpu.VMEM((num_rows, width), BF16),
            pltpu.VMEM((num_rows, width), BF16),
            pltpu.VMEM((nz, num_rows // ROW_BLOCK, share * ROW_BLOCK, head), F32),
            pltpu.VMEM((nz, num_rows // ROW_BLOCK, share * ROW_BLOCK, head), F32),
            pltpu.VMEM((nz, num_rows // ROW_BLOCK, share * ROW_BLOCK, head), F32),
            pltpu.VMEM((2 * heads, num_rows), F32),
            pltpu.VMEM((nz, share) + piece, F32),
            pltpu.VMEM((far, share) + piece, F32),
            pltpu.VMEM((far - 1, share) + piece, F32),
            pltpu.VMEM((group, share, num_rows, head), F32),
            pltpu.VMEM((num_rows, width), F32),
            pltpu.VMEM((2, num_rows, 2 * head), BF16),
            pltpu.VMEM((OUT_SLOTS, 2 * head, width), BF16),
            dma((1,)),
            dma((width // OUT_TILE,)),
            dma((2, nz)),
            dma((OUT_SLOTS, 2)),
            dma((2,)),
            dma((nz,)),
            dma((nz,)),
            dma((far, share)),
            dma((far, share)),
            dma((far - 1, share)),
            dma((far - 1, share)),
            dma((far, share)),
            dma((far, share)),
            dma((far - 1, share)),
            dma((far - 1, share)),
            dma((nz, share)),
            dma((nz, share)),
        ],
        compiler_params=pltpu.CompilerParams(collective_id=1, has_side_effects=True, vmem_limit_bytes=62 * MIB),
    )(stat, num, hidden, w_o)


def solution(mesh):
    group = mesh.shape['sp']

    def local_step(hidden, w_norm, w_q, w_k, w_v, w_o, k_block, v_block, cache_len):
        q, k_new, v_new = project(hidden, w_norm, w_q, w_k, w_v, cache_len)
        k_out, v_out, num, stat = attend(q, k_new, v_new, k_block, v_block, cache_len)
        out = combine(num, stat, hidden, w_o, group)
        return out, k_out, v_out

    cache_spec = P('dp', 'sp', None)
    return jax.shard_map(local_step, mesh=mesh, in_specs=(P('dp', None), P(None), P(None, None), P(None, None), P(None, None), P(None, None), cache_spec, cache_spec, P('dp')), out_specs=(P('dp', None), cache_spec, cache_spec), check_vma=False)
```

```python
import functools

import jax
import jax.numpy as jnp
import numpy as np
from jax import lax
from jax.experimental import pallas as pl
from jax.experimental.pallas import tpu as pltpu
from jax.sharding import PartitionSpec as P

ROPE_BASE = 10000.0
EPSILON = 1e-6
MIB = 1024 * 1024
F32 = jnp.float32
BF16 = jnp.bfloat16
FLOOR = float(np.finfo(np.float32).min)
MESH = pl.DeviceIdType.MESH
TURN = (6.28125, 0.0019340515136718750, float(2 * np.pi - 6.28125 - 0.0019340515136718750))
ROW_BLOCK = 8
OUT_SLOTS = 12
PROJ_WINDOW = 4
ATTEND_WINDOW = 3
ATTEND_BLOCKS = 2
OUT_TILE = 3072


def remote(src, dst, send_sem, recv_sem, device):
    return pltpu.make_async_remote_copy(src_ref=src, dst_ref=dst, send_sem=send_sem, recv_sem=recv_sem, device_id={'sp': device}, device_id_type=MESH)


def enter(devices):
    barrier = pltpu.get_barrier_semaphore()
    for device in devices:
        pl.semaphore_signal(barrier, inc=1, device_id={'sp': device}, device_id_type=MESH)
    pl.semaphore_wait(barrier, len(devices))


def project_kernel(freq_ref, len_ref, w_norm_ref, x_hbm, w_q_ref, w_k_ref, w_v_ref, q_ref, k_ref, v_ref, x_ref, x_norm, w_buf, q_buf, x_sem, w_sem, kv_sem, out_sem, send_sem, recv_sem):
    me = lax.axis_index('sp')
    core = me % 2
    partner = me + 1 - 2 * core
    num_rows, width = x_ref.shape
    head = k_ref.shape[1]
    half = q_ref.shape[1] // ROW_BLOCK // 2
    pair = 2 * head
    num_blocks = half // 2
    first_head = core * half

    def fetch(block):
        columns = pl.ds(pl.multiple_of((first_head + 2 * block) * head, pair), pair)
        return pltpu.make_async_copy(w_q_ref.at[:, columns], w_buf.at[block + 1], w_sem.at[block])

    fetch_k = pltpu.make_async_copy(w_k_ref, w_buf.at[0, :, pl.ds(0, head)], kv_sem.at[0])
    fetch_v = pltpu.make_async_copy(w_v_ref, w_buf.at[0, :, pl.ds(head, head)], kv_sem.at[1])
    fetch_x = pltpu.make_async_copy(x_hbm, x_ref, x_sem.at[0])
    fetch_x.start()
    fetch(0).start()
    fetch(1).start()

    gain = 1.0 + w_norm_ref[...].astype(F32)
    angles = jnp.broadcast_to(len_ref[...].astype(F32), (num_rows, num_rows)).T * freq_ref[...]
    turns = jnp.round(angles * (0.5 / np.pi))
    for part in TURN:
        angles = angles - turns * part
    cos_t = jnp.cos(angles)
    sin_t = jnp.where(lax.broadcasted_iota(jnp.int32, angles.shape, 1) < head // 2, -1.0, 1.0) * jnp.sin(angles)
    fetch_x.wait()
    for block in range(2, PROJ_WINDOW):
        fetch(block).start()

    def normalise(step, carry):
        rows = pl.ds(pl.multiple_of(step * 16, 16), 16)
        x = x_ref[rows, :].astype(F32)
        inv_rms = lax.rsqrt(jnp.mean(x * x, axis=-1, keepdims=True) + EPSILON)
        x_norm[rows, :] = (x * inv_rms * gain).astype(BF16)
        return carry

    lax.fori_loop(0, num_rows // 16, normalise, 0)

    def rotate(u):
        u = u.astype(BF16).astype(F32)
        return u * cos_t + pltpu.roll(u, head // 2, 1) * sin_t

    enter([partner])

    def heads_of(c, block):
        rows = pl.multiple_of((c * half + 2 * block) * ROW_BLOCK, 2 * ROW_BLOCK)
        return q_ref.at[:, pl.ds(rows, 2 * ROW_BLOCK), :]

    def keep(block):
        return pltpu.make_async_copy(q_buf.at[block], heads_of(core, block), out_sem.at[block])

    def send(block):
        return remote(q_buf.at[block], heads_of(core, block), send_sem.at[block], recv_sem.at[block], partner)

    def step(block, carry):
        @pl.when(block + PROJ_WINDOW < num_blocks)
        def _():
            fetch(block + PROJ_WINDOW).start()

        @pl.when(block + PROJ_WINDOW == num_blocks)
        def _():
            fetch_k.start()
            fetch_v.start()

        fetch(block).wait()
        product = jnp.dot(x_norm[...], w_buf[block + 1], preferred_element_type=F32)
        for i in range(2):
            q = (rotate(product[:, i * head:(i + 1) * head]) * head ** -0.5).astype(BF16).astype(F32)
            q_buf[block, :, i * ROW_BLOCK:(i + 1) * ROW_BLOCK, :] = q.reshape(num_rows // ROW_BLOCK, ROW_BLOCK, head)
        send(block).start()
        keep(block).start()
        return carry

    lax.fori_loop(0, num_blocks, step, 0)
    fetch_k.wait()
    fetch_v.wait()
    both = jnp.dot(x_norm[...], w_buf[0], preferred_element_type=F32)
    k_ref[...] = rotate(both[:, :head]).astype(BF16).astype(F32)
    v_ref[...] = both[:, head:].astype(BF16).astype(F32)

    def finish(block, carry):
        keep(block).wait()
        send(block).wait_send()
        other = heads_of(1 - core, block)
        remote(q_buf.at[block], other, send_sem.at[block], recv_sem.at[block], partner).wait_recv()
        return carry

    lax.fori_loop(0, num_blocks, finish, 0)


def project(hidden, w_norm, w_q, w_k, w_v, cache_len):
    num_rows, width = hidden.shape
    head = w_k.shape[1]
    heads = w_q.shape[1] // head
    inv_freq = ROPE_BASE ** (-np.arange(head // 2) * 2.0 / head)
    inv_freq = jnp.asarray(np.concatenate([inv_freq, inv_freq])[None, :], F32)
    vmem = pl.BlockSpec(memory_space=pltpu.VMEM)
    hbm = pl.BlockSpec(memory_space=pltpu.HBM)
    blocks = heads // 4
    return pl.pallas_call(
        project_kernel,
        name='project',
        out_shape=(jax.ShapeDtypeStruct((num_rows // ROW_BLOCK, heads * ROW_BLOCK, head), F32), jax.ShapeDtypeStruct((num_rows, head), F32), jax.ShapeDtypeStruct((num_rows, head), F32)),
        in_specs=[vmem, vmem, vmem, hbm, hbm, hbm, hbm],
        out_specs=(hbm, vmem, vmem),
        scratch_shapes=[
            pltpu.VMEM((num_rows, width), BF16),
            pltpu.VMEM((num_rows, width), BF16),
            pltpu.VMEM((blocks + 1, width, 2 * head), BF16),
            pltpu.VMEM((blocks, num_rows // ROW_BLOCK, 2 * ROW_BLOCK, head), F32),
            pltpu.SemaphoreType.DMA((1,)),
            pltpu.SemaphoreType.DMA((blocks,)),
            pltpu.SemaphoreType.DMA((2,)),
            pltpu.SemaphoreType.DMA((blocks,)),
            pltpu.SemaphoreType.DMA((blocks,)),
            pltpu.SemaphoreType.DMA((blocks,)),
        ],
        compiler_params=pltpu.CompilerParams(collective_id=0, has_side_effects=True, vmem_limit_bytes=60 * MIB),
    )(inv_freq, cache_len.reshape(1, -1), w_norm, hidden, w_q, w_k, w_v)


def attend_kernel(len_ref, k_new_ref, v_new_ref, q_hbm, k_hbm, v_hbm, k_out_hbm, v_out_hbm, num_hbm, stat_ref, q_ref, k_ref, v_ref, num_ref, scores_ref, factors_ref, in_sem, out_sem):
    num_rows, slots, head = k_ref.shape
    blocks = ATTEND_BLOCKS
    rows = ROW_BLOCK * blocks
    steps = num_rows // rows
    heads = stat_ref.shape[0] // 2
    base = lax.axis_index('sp') * slots
    group_iota = lax.broadcasted_iota(jnp.int32, (16, head), 0)
    lane_iota = lax.broadcasted_iota(jnp.int32, (heads, slots), 1)

    def loads(step):
        block = pl.ds(step * rows, rows)
        part = pl.ds(step * blocks, blocks)
        sem = in_sem.at[lax.rem(step, ATTEND_WINDOW + 1)]
        return [pltpu.make_async_copy(src, dst, sem) for src, dst in ((k_hbm.at[block], k_ref.at[block]), (v_hbm.at[block], v_ref.at[block]), (q_hbm.at[part], q_ref.at[part]))]

    def store_caches(step):
        block = pl.ds(step * rows, rows)
        return [pltpu.make_async_copy(src, dst, out_sem.at[0]) for src, dst in ((k_ref.at[block], k_out_hbm.at[block]), (v_ref.at[block], v_out_hbm.at[block]))]

    def store_partial(step):
        part = pl.ds(step * blocks, blocks)
        return pltpu.make_async_copy(num_ref.at[part], num_hbm.at[part], out_sem.at[0])

    def start(step, carry):
        for copy in loads(step):
            copy.start()
        return carry

    def attend_rows(step, carry):
        first = step * rows

        for copy in loads(step):
            copy.wait()

        @pl.when(step == 0)
        def _():
            start(ATTEND_WINDOW - 1, 0)

        @pl.when(step + ATTEND_WINDOW < steps)
        def _():
            start(step + ATTEND_WINDOW, 0)

        places = [len_ref[first + r] - base for r in range(rows)]
        for new, cache in ((k_new_ref, k_ref), (v_new_ref, v_ref)):
            fresh = new[pl.ds(pl.multiple_of(first, rows), rows), :]
            for r, p in enumerate(places):
                group = pl.multiple_of(jnp.clip(p, 0, slots - 1) // 16 * 16, 16)
                tile = cache[first + r, pl.ds(group, 16), :].astype(F32)
                cache[first + r, pl.ds(group, 16), :] = jnp.where(group_iota == p - group, fresh[r:r + 1, :], tile).astype(BF16)
        for r in range(rows):
            queries = q_ref.at[step * blocks + r // ROW_BLOCK]
            q = queries[pl.ds(r % ROW_BLOCK, heads, stride=ROW_BLOCK), :].astype(BF16)
            scores_ref[r] = lax.dot_general(q, k_ref[first + r], (((1,), (1,)), ((), ())), preferred_element_type=F32)
        for copy in store_caches(step):
            copy.start()
        stat_m = stat_ref[0:heads, :]
        stat_l = stat_ref[heads:2 * heads, :]
        for r, p in enumerate(places):
            valid = lane_iota <= p
            scores = jnp.where(valid, scores_ref[r], FLOOR)
            row_max = jnp.max(scores, axis=1, keepdims=True)
            weights = jnp.where(valid, jnp.exp(scores - row_max), 0.0)
            here = lane_iota == first + r
            stat_m = jnp.where(here, row_max, stat_m)
            stat_l = jnp.where(here, jnp.sum(weights, axis=1, keepdims=True), stat_l)
            factors_ref[r] = weights.astype(BF16)
        stat_ref[0:heads, :] = stat_m
        stat_ref[heads:2 * heads, :] = stat_l
        for r in range(rows):
            partial = num_ref.at[step * blocks + r // ROW_BLOCK]
            partial[pl.ds(r % ROW_BLOCK, heads, stride=ROW_BLOCK), :] = jnp.dot(factors_ref[r], v_ref[first + r], preferred_element_type=F32)
        store_partial(step).start()
        return carry

    def finish(step, carry):
        for copy in store_caches(step):
            copy.wait()
        store_partial(step).wait()
        return carry

    lax.fori_loop(0, ATTEND_WINDOW - 1, start, 0)
    lax.fori_loop(0, steps, attend_rows, 0)
    lax.fori_loop(0, steps, finish, 0)


def attend(q, k_new, v_new, k_block, v_block, cache_len):
    num_rows, slots, head = k_block.shape
    heads = q.shape[1] // ROW_BLOCK
    smem = pl.BlockSpec(memory_space=pltpu.SMEM)
    vmem = pl.BlockSpec(memory_space=pltpu.VMEM)
    hbm = pl.BlockSpec(memory_space=pltpu.HBM)
    return pl.pallas_call(
        attend_kernel,
        name='attend',
        out_shape=(jax.ShapeDtypeStruct(k_block.shape, BF16), jax.ShapeDtypeStruct(v_block.shape, BF16), jax.ShapeDtypeStruct(q.shape, F32), jax.ShapeDtypeStruct((2 * heads, num_rows), F32)),
        in_specs=[smem, vmem, vmem, hbm, hbm, hbm],
        out_specs=(hbm, hbm, hbm, vmem),
        scratch_shapes=[
            pltpu.VMEM(q.shape, F32),
            pltpu.VMEM(k_block.shape, BF16),
            pltpu.VMEM(v_block.shape, BF16),
            pltpu.VMEM(q.shape, F32),
            pltpu.VMEM((ATTEND_BLOCKS * ROW_BLOCK, heads, slots), F32),
            pltpu.VMEM((ATTEND_BLOCKS * ROW_BLOCK, heads, slots), BF16),
            pltpu.SemaphoreType.DMA((ATTEND_WINDOW + 1,)),
            pltpu.SemaphoreType.DMA((1,)),
        ],
        compiler_params=pltpu.CompilerParams(vmem_limit_bytes=60 * MIB),
    )(cache_len, k_new, v_new, q, k_block, v_block)


def combine_kernel(nz, stat_ref, num_ref, x_hbm, w_o_ref, out_hbm, x_ref, out_ref, own_num, sent_num, near_num, near_stat, part, from_long, from_short, gathered, total, attended, w_buf, x_sem, out_sem, own_sem, w_sem, stat_sem, near_send, near_recv, long_send, long_recv, short_send, short_recv, far_send, far_recv, back_send, back_recv, side_send, side_recv):
    me = lax.axis_index('sp')
    z = me // 2
    core = me % 2
    partner = me + 1 - 2 * core
    way = 1 - 2 * core
    num_rows, width = x_ref.shape
    heads = num_ref.shape[1] // ROW_BLOCK
    head = num_ref.shape[2]
    share = heads // (2 * nz)
    far = nz // 2

    def device(chip, c):
        return (chip + 2 * nz) % nz * 2 + c

    ahead = device(z + way, core)
    behind = device(z - way, core)
    targets = [far]
    for hop in range(far - 1, 0, -1):
        targets += [-hop, hop]
    targets.append(0)
    sources = [0]
    for hop in range(1, far):
        sources += [-hop, hop]
    sources.append(-far)

    units = [(0, s) for s in range(share)]
    for hop in range(1, far):
        units += [(sources.index(step), s) for s in range(share) for step in (-hop, hop)]
    units += [(nz - 1, s) for s in range(share)]

    def fetch(u):
        k, s = units[u]
        chip = z + way * sources[k]
        rows = [pl.ds(pl.multiple_of((device(chip, c) * share + s) * head, head), head) for c in range(2)]
        return [pltpu.make_async_copy(w_o_ref.at[rows[c], :], w_buf.at[u % OUT_SLOTS, c * head:(c + 1) * head, :], w_sem.at[u % OUT_SLOTS, c]) for c in range(2)]

    def start_fetch(u):
        for copy in fetch(u):
            copy.start()

    def own_heads(i, c):
        way_c = way * (1 - 2 * c)
        rows = share * ROW_BLOCK
        first = rows * device(z + way_c * targets[i], core + way * c)
        return num_ref.at[:, pl.ds(pl.multiple_of(first, rows), rows), :]

    def stage(i):
        return [pltpu.make_async_copy(own_heads(i, 1), sent_num.at[i], own_sem.at[1, i]), pltpu.make_async_copy(own_heads(i, 0), own_num.at[i], own_sem.at[0, i])]

    stages = [stage(i) for i in range(nz)]
    swap_stat = remote(stat_ref, near_stat, stat_sem.at[0], stat_sem.at[1], partner)
    swaps = [remote(sent_num.at[i], near_num.at[i], near_send.at[i], near_recv.at[i], partner) for i in range(nz)]

    def start_swaps(low, high):
        for i in range(low, high):
            stages[i][0].wait()
            swaps[i].start()

    for i in range(2):
        for copy in stages[i]:
            copy.start()
    enter([partner, ahead, behind])
    swap_stat.start()
    start_swaps(0, 2)
    for i in range(2, nz):
        for copy in stages[i]:
            copy.start()
    start_swaps(2, 4)
    fetch_x = pltpu.make_async_copy(x_hbm, x_ref, x_sem.at[0])
    ahead_of_use = list(range(OUT_SLOTS))

    def fetch_some(count):
        for _ in range(count):
            if ahead_of_use:
                start_fetch(ahead_of_use.pop(0))

    def column(row):
        return jnp.broadcast_to(row, (num_rows, num_rows)).T

    def merge(a, b):
        (x_a, m_a, l_a), (x_b, m_b, l_b) = a, b
        m = jnp.maximum(m_a, m_b)
        scale_a = jnp.exp(m_a - m)
        scale_b = jnp.exp(m_b - m)
        return x_a * column(scale_a) + x_b * column(scale_b), m, l_a * scale_a + l_b * scale_b

    def load(ref):
        return ref[0:num_rows, :], ref[num_rows:num_rows + 1, :], ref[num_rows + 1:num_rows + 2, :]

    sub_iota = lax.broadcasted_iota(jnp.int32, (8, num_rows), 0)

    def store(ref, triple):
        x, m, l = triple
        ref[0:num_rows, :] = x
        ref[num_rows:num_rows + 8, :] = jnp.where(sub_iota == 0, m, l)

    def own(i, send=None):
        stages[i][1].wait()
        swaps[i].wait_recv()
        first = share * device(z + way * targets[i], core)
        for s in range(share):
            h = first + s
            rows = slice(s * ROW_BLOCK, (s + 1) * ROW_BLOCK)
            mine = (own_num[i, :, rows, :].reshape(num_rows, head), stat_ref[pl.ds(h, 1), :], stat_ref[pl.ds(heads + h, 1), :])
            theirs = (near_num[i, :, rows, :].reshape(num_rows, head), near_stat[pl.ds(h, 1), :], near_stat[pl.ds(heads + h, 1), :])
            store(part.at[i, s], merge(mine, theirs))
            if send is not None:
                send(0, s).start()

    def long_copy(hop, s):
        i = 0 if hop == 0 else 2 * hop
        return remote(part.at[i, s], from_long.at[hop, s], long_send.at[hop, s], long_recv.at[hop, s], ahead)

    def short_copy(hop, s):
        return remote(part.at[2 * hop + 1, s], from_short.at[hop, s], short_send.at[hop, s], short_recv.at[hop, s], behind)

    swap_stat.wait_recv()
    for hop in range(far):
        if hop == 0:
            own(0, long_copy)
            own(1, short_copy)
            start_swaps(4, nz)
            fetch_x.start()
            fetch_some(2)
            continue
        own(2 * hop)
        own(2 * hop + 1)
        for s in range(share):
            long_copy(hop - 1, s).wait_recv()
            store(part.at[2 * hop, s], merge(load(part.at[2 * hop, s]), load(from_long.at[hop - 1, s])))
            long_copy(hop, s).start()
            fetch_some(2)
            if hop < far - 1:
                short_copy(hop - 1, s).wait_recv()
                store(part.at[2 * hop + 1, s], merge(load(part.at[2 * hop + 1, s]), load(from_short.at[hop - 1, s])))
                short_copy(hop, s).start()

    def far_copy(hop, s):
        slot = gathered.at[device(z - way * hop, core), s]
        return remote(slot, slot, far_send.at[hop, s], far_recv.at[hop, s], ahead)

    def back_copy(hop, s):
        slot = gathered.at[device(z + way * hop, core), s]
        return remote(slot, slot, back_send.at[hop, s], back_recv.at[hop, s], behind)

    def side_copy(k, s):
        slot = gathered.at[device(z + way * sources[k], core), s]
        return remote(slot, slot, side_send.at[k, s], side_recv.at[k, s], partner)

    def far_arrival(hop, s):
        slot = gathered.at[device(z - way * (hop + 1), core), s]
        return remote(slot, slot, far_send.at[hop, s], far_recv.at[hop, s], ahead)

    def back_arrival(hop, s):
        slot = gathered.at[device(z + way * (hop + 1), core), s]
        return remote(slot, slot, back_send.at[hop, s], back_recv.at[hop, s], behind)

    def side_arrival(k, s):
        slot = gathered.at[device(z - way * sources[k], 1 - core), s]
        return remote(slot, slot, side_send.at[k, s], side_recv.at[k, s], partner)

    mirror = {hop: k for k, hop in enumerate(sources)}
    mirror[far] = mirror[-far]

    last = far - 1
    fetch_some(OUT_SLOTS)
    for s in range(share):
        short_copy(last - 1, s).wait_recv()
        triple = merge(load(part.at[2 * far - 1, s]), load(from_short.at[last - 1, s]))
        long_copy(last, s).wait_recv()
        x, _, l = merge(triple, load(from_long.at[last, s]))
        gathered[me, s] = (x / column(l)).astype(BF16).astype(F32)
        far_copy(0, s).start()
        back_copy(0, s).start()
        side_copy(0, s).start()

    tiles = width // OUT_TILE
    start = me // (2 * nz)

    def save(n):
        columns = pl.ds(pl.multiple_of(n * OUT_TILE, OUT_TILE), OUT_TILE)
        return pltpu.make_async_copy(out_ref.at[:, columns], out_hbm.at[:, columns], out_sem.at[n])

    def multiply(us):
        for i, u in enumerate(us):
            k, s = units[u]
            side_arrival(mirror[-sources[k]], s).wait_recv()
            chip = z + way * sources[k]
            for c in range(2):
                attended[i, :, c * head:(c + 1) * head] = gathered[device(chip, c), s].astype(BF16)
            for copy in fetch(u):
                copy.wait()

        def tile(n, carry):
            columns = pl.ds(pl.multiple_of((start + n) * OUT_TILE, OUT_TILE), OUT_TILE)
            product = None
            for i, u in enumerate(us):
                term = jnp.dot(attended[i], w_buf[u % OUT_SLOTS, :, columns], preferred_element_type=F32)
                product = term if product is None else product + term
            before = x_ref[:, columns].astype(F32) if 0 in us else total[:, columns]
            if len(units) - 1 in us:
                out_ref[:, columns] = (before + product).astype(BF16)
                save(n).start()
            else:
                total[:, columns] = before + product
            return carry

        for n in range(tiles):
            tile(n, 0)
        for u in us:
            if u + OUT_SLOTS < len(units):
                start_fetch(u + OUT_SLOTS)

    chunks = [[s] for s in range(share)]
    while sum(map(len, chunks)) < len(units) - share:
        u = sum(map(len, chunks))
        chunks.append([u, u + 1])
    chunks += [[len(units) - share + s] for s in range(share)]
    fetch_x.wait()
    multiply(chunks.pop(0))
    multiply(chunks.pop(0))
    swap_stat.wait_send()
    for swap in swaps:
        swap.wait_send()
    for s in range(share):
        for hop in range(far):
            long_copy(hop, s).wait_send()
            if hop < far - 1:
                short_copy(hop, s).wait_send()
    for hop in range(far):
        for s in range(share):
            far_arrival(hop, s).wait_recv()
            if hop < far - 1:
                far_copy(hop + 1, s).start()
            side_copy(mirror[-(hop + 1)], s).start()
            if hop < far - 1:
                back_arrival(hop, s).wait_recv()
                if hop < far - 2:
                    back_copy(hop + 1, s).start()
                side_copy(mirror[hop + 1], s).start()
            multiply(chunks.pop(0))
    for chunk in chunks:
        multiply(chunk)
    for n in range(tiles):
        save(n).wait()

    for s in range(share):
        for hop in range(far):
            far_copy(hop, s).wait_send()
            if hop < far - 1:
                back_copy(hop, s).wait_send()
        for k in range(nz):
            side_copy(k, s).wait_send()


def combine(num, stat, hidden, w_o, group):
    num_rows, width = hidden.shape
    heads = num.shape[1] // ROW_BLOCK
    head = num.shape[2]
    nz = group // 2
    share = heads // group
    far = nz // 2
    vmem = pl.BlockSpec(memory_space=pltpu.VMEM)
    hbm = pl.BlockSpec(memory_space=pltpu.HBM)
    dma = pltpu.SemaphoreType.DMA
    piece = (num_rows + 8, head)
    return pl.pallas_call(
        functools.partial(combine_kernel, nz),
        name='combine',
        out_shape=jax.ShapeDtypeStruct((num_rows, width), BF16),
        in_specs=[vmem, hbm, hbm, hbm],
        out_specs=hbm,
        scratch_shapes=[
            pltpu.VMEM((num_rows, width), BF16),
            pltpu.VMEM((num_rows, width), BF16),
            pltpu.VMEM((nz, num_rows // ROW_BLOCK, share * ROW_BLOCK, head), F32),
            pltpu.VMEM((nz, num_rows // ROW_BLOCK, share * ROW_BLOCK, head), F32),
            pltpu.VMEM((nz, num_rows // ROW_BLOCK, share * ROW_BLOCK, head), F32),
            pltpu.VMEM((2 * heads, num_rows), F32),
            pltpu.VMEM((nz, share) + piece, F32),
            pltpu.VMEM((far, share) + piece, F32),
            pltpu.VMEM((far - 1, share) + piece, F32),
            pltpu.VMEM((group, share, num_rows, head), F32),
            pltpu.VMEM((num_rows, width), F32),
            pltpu.VMEM((2, num_rows, 2 * head), BF16),
            pltpu.VMEM((OUT_SLOTS, 2 * head, width), BF16),
            dma((1,)),
            dma((width // OUT_TILE,)),
            dma((2, nz)),
            dma((OUT_SLOTS, 2)),
            dma((2,)),
            dma((nz,)),
            dma((nz,)),
            dma((far, share)),
            dma((far, share)),
            dma((far - 1, share)),
            dma((far - 1, share)),
            dma((far, share)),
            dma((far, share)),
            dma((far - 1, share)),
            dma((far - 1, share)),
            dma((nz, share)),
            dma((nz, share)),
        ],
        compiler_params=pltpu.CompilerParams(collective_id=1, has_side_effects=True, vmem_limit_bytes=62 * MIB),
    )(stat, num, hidden, w_o)


def solution(mesh):
    group = mesh.shape['sp']

    def local_step(hidden, w_norm, w_q, w_k, w_v, w_o, k_block, v_block, cache_len):
        q, k_new, v_new = project(hidden, w_norm, w_q, w_k, w_v, cache_len)
        k_out, v_out, num, stat = attend(q, k_new, v_new, k_block, v_block, cache_len)
        out = combine(num, stat, hidden, w_o, group)
        return out, k_out, v_out

    cache_spec = P('dp', 'sp', None)
    return jax.shard_map(local_step, mesh=mesh, in_specs=(P('dp', None), P(None), P(None, None), P(None, None), P(None, None), P(None, None), cache_spec, cache_spec, P('dp')), out_specs=(P('dp', None), cache_spec, cache_spec), check_vma=False)
```
